512 devices in a mesh: sector: 32 (over z, core), cap: 16 (over y, x).
Axes of the slice: x: 4, y: 4, z: 16, core: 2. Of those that a mesh axis runs over, the one named last changes fastest.
Arguments:
- start_value: float32 [256, 32, 2048], P('sector', None, 'cap'), may hold values from 0 to 4
- firm_mass: float32 [256, 32, 2048], P('sector', None, 'cap'), may hold values from 0.1 to 10
- survive: int32 [256, 32, 2048], P('sector', None, 'cap'), may hold values from 0 to 1, as said below
- exit_index: int32 [256], P('sector'), may hold values from 0 to 8
- demand: float32 [256], P('sector'), may hold values from 0.3 to 90, as said below
- transition: float32 [32, 32], replicated, may hold values from 0 to 1, as said below
- install_cost: float32 [2048], P('cap'), may hold values from 0 to 1
Outputs:
- final_value: float32 [256, 32, 2048], P('sector', None, 'cap')
- rel_prices: float32 [256], P('sector')
The draws below stay inside these ranges and needn't reach their ends.
Inputs may be any that keep to these rules, and one draw needn't show every extreme that they name: `survive`: 0 or 1; the share of ones differs from sector to sector, from about a tenth to all. `demand`: positive, rising over the sectors by some thirty times. `transition`: entries positive, every row sums to one.
All inputs are finite; a program needn't handle non-finite values.
Results may differ from the reference program's by a relative error of at most 0.0003.
Values sent between devices are 32-bit elements; how exact they have to be, the bound alone decides.
A program may use at most 64 MiB of HBM per device.

```python
import math
import jax
import jax.numpy as jnp
from jax import lax

K = 2048
Z = 32
SWEEPS = 2
S = 256


def draw_survive(key, part):
    first_key, second_key = jax.random.split(jax.random.fold_in(key, 11))
    shares = jax.random.randint(first_key, (S, 1, 1), 10, 101)
    rolled = jax.random.randint(second_key, (S, Z, K), 0, 100)
    return (rolled < shares).astype(jnp.int32)


def draw_demand(key, part):
    sector_pos = jnp.arange(S).astype(jnp.float32)
    base = jnp.exp(jnp.log(30.0) * sector_pos / max(S - 1, 1))
    noise = jax.random.uniform(jax.random.fold_in(key, 21), (S,), minval=-0.5, maxval=0.5)
    return (base * jnp.exp(noise)).astype(jnp.float32)


def draw_transition(key, part):
    states = jnp.arange(Z)
    spread = jnp.abs(states[:, None] - states[None, :]).astype(jnp.float32)
    raw = jax.random.uniform(jax.random.fold_in(key, 31), (Z, Z), minval=0.3, maxval=1.0) * jnp.exp(-spread / 4.0)
    raw = raw + jnp.eye(Z, dtype=jnp.float32)
    return (raw / jnp.sum(raw, axis=1, keepdims=True)).astype(jnp.float32)


def touch_ends(values, own_key, smallest, top_value):
    shape = values.shape
    spot = [jax.random.randint(jax.random.fold_in(own_key, axis), (), 0, shape[axis]) for axis in range(len(shape))]
    values = values.at[tuple(spot)].set(smallest)
    longest = shape.index(max(shape))
    spot[longest] = (spot[longest] + 1) % shape[longest]
    return values.at[tuple(spot)].set(top_value)


def levels(own_key, dims, cuts, least, high):
    loudness, own = 1.0, jax.random.fold_in(own_key, 6)
    for position, blocks in cuts:
        steps = jnp.exp(jax.random.uniform(jax.random.fold_in(own, position), (blocks,), jnp.float32, least / len(cuts), high / len(cuts)))
        loudness = loudness * jnp.repeat(steps, dims[position] // blocks).reshape([-1 if axis == position else 1 for axis in range(len(dims))])
    return loudness


def setup_inputs(seed: int = 0) -> dict:
    arg_keys = jax.random.split(jax.random.key(seed), 8)
    start_value = jnp.clip(4.0 * jax.random.uniform(arg_keys[0], (S, Z, K), jnp.float32) ** levels(arg_keys[0], (S, Z, K), ((0, 32), (2, 16)), -0.2, 0.2), 0.0, 4.0)
    firm_mass = jnp.clip(jnp.exp(math.log(10.0) - 4.6051702 * jax.random.uniform(arg_keys[1], (S, Z, K), jnp.float32) ** levels(arg_keys[1], (S, Z, K), ((0, 32), (2, 16)), -0.2, 0.2)), 0.1, 10.0)
    survive = draw_survive(jax.random.fold_in(arg_keys[7], 71), 0)
    exit_index = touch_ends(jax.random.randint(arg_keys[3], (S,), 0, Z // 4 + 1), jax.random.fold_in(arg_keys[3], 1), 0, (Z // 4 + 1) - 1).astype(jnp.int32)
    demand = draw_demand(jax.random.fold_in(arg_keys[7], 71), 0)
    transition = draw_transition(jax.random.fold_in(arg_keys[7], 71), 0)
    install_cost = jnp.clip(1.0 * jax.random.uniform(arg_keys[6], (K,), jnp.float32) ** levels(arg_keys[6], (K,), ((0, 16),), -0.2, 0.2), 0.0, 1.0)
    return dict(start_value=start_value, firm_mass=firm_mass, survive=survive, exit_index=exit_index, demand=demand, transition=transition, install_cost=install_cost)


def capital_of(positions):
    return 0.2 * jnp.exp(jnp.log(10.0) * positions.astype(jnp.float32) / (K - 1))

def charge_of(cap_now, cap_next, row_ids, col_ids):
    invest = cap_next - 0.9 * cap_now
    fixed = jnp.where(row_ids == col_ids, 0.0, 1.5 * cap_now)
    return invest + invest * invest / cap_now + fixed

def sector_best(forward_value):
    row_block = math.gcd(K, 256)
    col_ids = jnp.arange(K, dtype=jnp.int32)
    capital = capital_of(col_ids)

    def row_step(first_row):
        row_ids = first_row + jnp.arange(row_block, dtype=jnp.int32)
        rows = capital_of(row_ids)
        charge = charge_of(rows[:, None], capital[None, :], row_ids[:, None], col_ids[None, :])
        return lax.optimization_barrier(jnp.max(forward_value[:, None, :] - charge[None], axis=2))
    starts = (jnp.arange(K // row_block) * row_block).astype(jnp.int32)
    blocks = lax.map(row_step, starts)
    return blocks.transpose(1, 0, 2).reshape(Z, K)

def reference(start_value, firm_mass, survive, exit_index, demand, transition, install_cost):
    prod_index = jnp.arange(Z, dtype=jnp.int32)
    capital = capital_of(jnp.arange(K, dtype=jnp.int32))
    log_prod = -0.5 + prod_index.astype(jnp.float32) / (Z - 1)
    output = jnp.exp(log_prod)[:, None] * capital[None, :] ** 0.6
    scrap = 0.3 * capital
    live = (survive == 1) & (prod_index[None, :, None] >= exit_index[:, None, None])
    values = start_value
    relative = jnp.zeros((S,), jnp.float32)
    for sweep in range(SWEEPS):
        staying = jnp.where(live, jax.nn.sigmoid((values - scrap) / 0.5), 0.0)
        supply = 1.0 + lax.optimization_barrier(jnp.sum(firm_mass * staying * output, axis=(1, 2))) / (Z * K)
        prices = jnp.sqrt(demand / supply)
        price_index = jnp.mean(jnp.sqrt(prices)) ** 2
        relative = prices / price_index
        continuation = jnp.where(live, jnp.maximum(values, scrap), scrap)
        expect = jnp.einsum('zw,swk->szk', transition, continuation, precision=lax.Precision.HIGHEST)
        forward_value = 0.9 * expect - install_cost[None, None, :]
        best = lax.map(sector_best, forward_value)
        values = jnp.where(live, relative[:, None, None] * output + best, scrap)
    return (values, relative)
```

```python
import math

import jax
import jax.numpy as jnp
import numpy as np
from jax import lax
from jax.experimental import pallas as pl
from jax.experimental.pallas import tpu as pltpu
from jax.sharding import PartitionSpec as P

K = 2048
Z = 32
SWEEPS = 2
SEC = 8
CAPS = 16
ZS = 16
ROWS = 16
CHUNK = 32
CHUNKS = K // CHUNK
STEPS = CHUNKS + CAPS - 1
GROUPS = K // 8
LINES = GROUPS + 8 * (CAPS - 1)
SHIFT = 8 * (CAPS - 1)
ENDS = 96
NEG = -1e30
LOG10 = float(np.log(np.float32(10.0)))


def capital_of(positions):
    return 0.2 * jnp.exp(LOG10 * positions.astype(jnp.float32) / (K - 1))


def iota(shape, axis):
    return lax.broadcasted_iota(jnp.int32, shape, axis)


def kernel(
    exit_ref, demand_ref, start_ref, mass_ref, survive_ref, trans_ref, install_ref,
    value_ref, rel_ref,
    forward, heard, heights, lines, table, jumps, table_s, jumps_s,
    reached, folded, reply, best, part, parts, root, pair, both, roots,
    fwd_send, fwd_recv, rep_send, rep_recv, par_send, par_recv, pair_send, pair_recv,
    root_send, root_recv, table_sem,
):
    me = lax.axis_index("cap")
    sec = lax.axis_index("sector")
    core = lax.rem(sec, 2)
    level = sec // 2
    partner = sec + 1 - 2 * core

    def cap_at(d):
        return {"cap": lax.rem(me + d, CAPS)}

    def level_at(d):
        return {"sector": 2 * lax.rem(level + d, ZS) + core}

    barrier = pltpu.get_barrier_semaphore()

    def greet(d, c):
        pl.semaphore_signal(barrier, inc=1, device_id=cap_at(d))
        pl.semaphore_signal(barrier, inc=1, device_id=level_at(d))
        return c

    lax.fori_loop(1, CAPS, greet, 0)
    pl.semaphore_signal(barrier, inc=1, device_id={"sector": partner})

    capital_all = capital_of(iota((CAPS, 128), 0) * 128 + iota((CAPS, 128), 1))
    half = 0.8 * capital_all
    square_all = capital_all * capital_all
    low = iota((8, 128), 1) % 8
    own_place = 2 * low - 8 * (iota((8, 128), 1) // 8) - iota((8, 128), 0)

    def fill(i, c):
        lines[i] = capital_of(16 * (i - SHIFT) + own_place)
        return c

    lax.fori_loop(0, LINES, fill, 0, unroll=8)
    place = me * 128 + iota((1, 128), 1)
    capital = capital_of(place)
    scrap = 0.3 * capital
    log_cap = math.log(0.2) + LOG10 * place.astype(jnp.float32) / (K - 1)
    log_prod = -0.5 + iota((Z, 128), 0).astype(jnp.float32) / (Z - 1)
    output = jnp.exp(log_prod + 0.6 * log_cap)
    install = install_ref[...]
    lane = iota((ROWS, 128), 1)
    lane_f = lane.astype(jnp.float32)

    def fwd_copy(sweep, d):
        peer = lax.rem(me + d, CAPS)
        return pltpu.make_async_remote_copy(
            forward.at[sweep, peer], heard.at[sweep, me], fwd_send.at[sweep, d], fwd_recv.at[sweep, d],
            device_id=cap_at(d))

    def rep_copy(sweep, d):
        peer = lax.rem(me + d, CAPS)
        return pltpu.make_async_remote_copy(
            reply.at[sweep, peer], best.at[sweep, me], rep_send.at[sweep, d], rep_recv.at[sweep, d],
            device_id=cap_at(d))

    def par_copy(sweep, d):
        return pltpu.make_async_remote_copy(
            part.at[sweep], parts.at[sweep, me], par_send.at[sweep, d], par_recv.at[sweep, d],
            device_id=cap_at(d))

    def root_copy(sweep, d):
        return pltpu.make_async_remote_copy(
            both.at[sweep], roots.at[sweep, level], root_send.at[sweep, d], root_recv.at[sweep, d],
            device_id=level_at(d))

    def start_all(copy, sweep):
        def one(d, c):
            copy(sweep, d).start()
            return c
        lax.fori_loop(1, CAPS, one, 0)

    def wait_all(copy, sweep):
        def one(d, c):
            copy(sweep, d).wait()
            return c
        lax.fori_loop(1, CAPS, one, 0)

    value_ref[...] = start_ref[...]

    def sweep_body(sweep, carry):
        sums = []
        for s in range(SEC):
            live = (survive_ref[s] == 1) & (iota((Z, 128), 0) >= exit_ref[s])
            values = value_ref[s]
            staying = jnp.where(live, jax.nn.sigmoid((values - scrap) * 2.0), 0.0)
            sums.append(jnp.sum(mass_ref[s] * staying * output, axis=0, keepdims=True))
            continuation = jnp.where(live, jnp.maximum(values, scrap), scrap)
            expect = lax.dot_general(
                trans_ref[...], continuation, (((1,), (0,)), ((), ())),
                precision=lax.Precision.HIGHEST, preferred_element_type=jnp.float32)
            ahead = 0.9 * expect - install
            forward[sweep, 2 * s] = ahead[:ROWS]
            forward[sweep, 2 * s + 1] = ahead[ROWS:]
        part[sweep] = jnp.concatenate(sums, axis=0)

        @pl.when(sweep == 0)
        def _():
            pl.semaphore_wait(barrier, CAPS - 1 + ZS - 1 + 1)

        start_all(par_copy, sweep)
        start_all(fwd_copy, sweep)
        heard[sweep, me] = forward[sweep, me]
        parts[sweep, me] = part[sweep]
        wait_all(par_copy, sweep)
        whole = jnp.sum(jnp.sum(parts[sweep], axis=0), axis=1, keepdims=True)
        supply = 1.0 + jnp.broadcast_to(whole, (SEC, 128)) / (Z * K)
        demand = jnp.zeros((SEC, 128), jnp.float32)
        for s in range(SEC):
            demand = jnp.where(iota((SEC, 128), 0) == s, demand_ref[s], demand)
        prices = jnp.sqrt(demand / supply)
        root[sweep] = jnp.sum(jnp.sqrt(prices), axis=0, keepdims=True)
        to_pair = pltpu.make_async_remote_copy(
            root.at[sweep], pair.at[sweep], pair_send.at[sweep], pair_recv.at[sweep],
            device_id={"sector": partner})
        to_pair.start()
        to_pair.wait()
        both[sweep] = root[sweep] + pair[sweep]
        start_all(root_copy, sweep)
        roots[sweep, level] = both[sweep]

        wait_all(fwd_copy, sweep)

        def spread(i, c):
            rows = [heard[sweep, i] + 0.8 * capital_of(i * 128 + iota((1, 128), 1))]
            for bit in (64, 32, 16, 8):
                high = (lane // bit) % 2 == 1
                wide = []
                for x in rows:
                    turned = pltpu.roll(x, bit, 1)
                    wide += [jnp.where(high, turned, x), jnp.where(high, x, turned)]
                rows = wide
            for g in range(16):
                heights[16 * i + g] = rows[g]
            return c

        lax.fori_loop(0, CAPS, spread, 0)

        tall = heard[sweep] + half[:, None, :]
        source = lax.broadcasted_iota(jnp.int32, (CAPS, ROWS, 128), 0).astype(jnp.float32)
        chunks = []
        for b in range(1, CAPS):
            rate = 1.0 / (0.2 * math.exp(LOG10 * 128 * b / (K - 1)))
            here = tall - (square_all * rate)[:, None, :]
            top = jnp.max(here, axis=0)
            where = jnp.min(jnp.where(here == top[None], source, 1e9), axis=0)
            peak = jnp.max(top, axis=1, keepdims=True)
            spot = where * (128 // CHUNK) + (lane // CHUNK).astype(jnp.float32)
            chunk = jnp.min(jnp.where(top == peak, spot, 1e9), axis=1, keepdims=True)
            chunk = jnp.broadcast_to(chunk, (ROWS, 128))
            chunks.append(jnp.maximum(chunk, chunks[-1]) if chunks else chunk)
        chunks.append(jnp.full((ROWS, 128), float(CHUNKS - 1), jnp.float32))
        block = jnp.zeros((ROWS, 128), jnp.float32)
        jump = jnp.zeros((ROWS, 128), jnp.float32)
        for b in range(1, CAPS):
            first = chunks[b - 1] + float(b)
            block = block + jnp.where(first <= lane_f, 1.0, 0.0)
            jump = jnp.where(first == lane_f, NEG, jump)
        group = 4.0 * (lane_f - block)
        line = group - 8.0 * block + float(SHIFT)
        for b in range(CAPS):
            group = jnp.where(lane == ENDS + b, chunks[b] + float(b), group)
        table[:ROWS] = jnp.clip(group.astype(jnp.int32), 0, jnp.where(lane < ENDS, GROUPS - 4, STEPS - 1))
        table[ROWS:] = jnp.clip(line.astype(jnp.int32), 0, LINES - 4)
        jumps[...] = jump
        to_table = pltpu.make_async_copy(table, table_s, table_sem.at[0])
        to_jumps = pltpu.make_async_copy(jumps, jumps_s, table_sem.at[1])
        to_table.start()
        to_jumps.start()
        to_table.wait()
        to_jumps.wait()

        def step(t, accs):
            out = []
            for r in range(ROWS):
                at_height = jnp.clip(table_s[r, t], 0, GROUPS - 4)
                at_line = jnp.clip(table_s[ROWS + r, t], 0, LINES - 4)
                value = heights[pl.ds(at_height, 4), r:r + 1, :] - lines[pl.ds(at_line, 4)]
                acc = jnp.maximum(jnp.max(value, axis=0), accs[r] + jumps_s[r, t])
                reached[r, t] = acc
                out.append(acc)
            return tuple(out)

        lax.fori_loop(0, STEPS, step, tuple(jnp.full((8, 128), NEG, jnp.float32) for _ in range(ROWS)))

        for h in range(2):
            odd = iota((ROWS * 8, 128), 1)
            tops = []
            for p in range(8):
                tops.append(jnp.concatenate(
                    [reached[r, jnp.clip(table_s[r, ENDS + 8 * h + p], 0, STEPS - 1)] for r in range(ROWS)], axis=0))
            for bit in (4, 2, 1):
                high = (odd // bit) % 2 == 1
                less = []
                for i in range(len(tops) // 2):
                    x, y = tops[i], tops[i + len(tops) // 2]
                    mine = jnp.where(high, y, x)
                    other = jnp.where(high, x, y)
                    other = jnp.where(high, pltpu.roll(other, bit, 1), pltpu.roll(other, 128 - bit, 1))
                    less.append(jnp.maximum(mine, other))
                tops = less
            folded[h] = tops[0].reshape(ROWS, 8, 128)
            ways = [folded[h, :, q, :] for q in range(8)]
            for bit in (4, 2, 1):
                high = (lane // bit) % 2 == 1
                for q in range(8):
                    if q & bit == 0:
                        x, y = ways[q], ways[q + bit]
                        ways[q] = jnp.where(high, pltpu.roll(y, bit, 1), x)
                        ways[q + bit] = jnp.where(high, y, pltpu.roll(x, 128 - bit, 1))
            for p in range(8):
                reply[sweep, 8 * h + p] = ways[p]
        start_all(rep_copy, sweep)
        best[sweep, me] = reply[sweep, me]
        wait_all(root_copy, sweep)
        root_sum = jnp.sum(roots[sweep], axis=0)
        price_index = root_sum / (SEC * 2 * ZS)
        price_index = price_index * price_index
        relative = prices / price_index
        wait_all(rep_copy, sweep)
        for s in range(SEC):
            for h in range(2):
                top = best[sweep, 2 * s + h] - 1.41 * capital
                stay = forward[sweep, 2 * s + h] - 0.11 * capital
                gain = jnp.maximum(top, stay)
                rows = slice(h * ROWS, (h + 1) * ROWS)
                live = (survive_ref[s, rows] == 1) & (iota((ROWS, 128), 0) + h * ROWS >= exit_ref[s])
                value_ref[s, rows] = jnp.where(live, relative[s:s + 1] * output[rows] + gain, scrap)
        flat = jnp.where(iota((SEC, 128), 0) == iota((SEC, 128), 1), relative, 0.0)
        rel_ref[...] = jnp.sum(flat, axis=0, keepdims=True)[:, :SEC]
        return carry

    lax.fori_loop(0, SWEEPS, sweep_body, 0)


def on_device(start_value, firm_mass, survive, exit_index, demand, transition, install_cost):
    f32 = jnp.float32
    vmem = pl.BlockSpec(memory_space=pltpu.VMEM)
    smem = pl.BlockSpec(memory_space=pltpu.SMEM)
    dma = pltpu.SemaphoreType.DMA
    values, relative = pl.pallas_call(
        kernel,
        out_shape=(jax.ShapeDtypeStruct((SEC, Z, 128), f32), jax.ShapeDtypeStruct((1, SEC), f32)),
        in_specs=[smem, smem, vmem, vmem, vmem, vmem, vmem],
        out_specs=(vmem, vmem),
        scratch_shapes=[
            pltpu.VMEM((SWEEPS, CAPS, ROWS, 128), f32),
            pltpu.VMEM((SWEEPS, CAPS, ROWS, 128), f32),
            pltpu.VMEM((GROUPS, ROWS, 128), f32),
            pltpu.VMEM((LINES, 8, 128), f32),
            pltpu.VMEM((2 * ROWS, 128), jnp.int32),
            pltpu.VMEM((ROWS, 128), f32),
            pltpu.SMEM((2 * ROWS, 128), jnp.int32),
            pltpu.SMEM((ROWS, 128), f32),
            pltpu.VMEM((ROWS, STEPS, 8, 128), f32),
            pltpu.VMEM((2, ROWS, 8, 128), f32),
            pltpu.VMEM((SWEEPS, CAPS, ROWS, 128), f32),
            pltpu.VMEM((SWEEPS, CAPS, ROWS, 128), f32),
            pltpu.VMEM((SWEEPS, SEC, 128), f32),
            pltpu.VMEM((SWEEPS, CAPS, SEC, 128), f32),
            pltpu.VMEM((SWEEPS, 1, 128), f32),
            pltpu.VMEM((SWEEPS, 1, 128), f32),
            pltpu.VMEM((SWEEPS, 1, 128), f32),
            pltpu.VMEM((SWEEPS, ZS, 1, 128), f32),
            dma((SWEEPS, CAPS)), dma((SWEEPS, CAPS)), dma((SWEEPS, CAPS)), dma((SWEEPS, CAPS)),
            dma((SWEEPS, CAPS)), dma((SWEEPS, CAPS)), dma((SWEEPS,)), dma((SWEEPS,)),
            dma((SWEEPS, ZS)), dma((SWEEPS, ZS)), dma((2,)),
        ],
        compiler_params=pltpu.CompilerParams(
            collective_id=0, has_side_effects=True, vmem_limit_bytes=40 << 20),
    )(exit_index, demand, start_value, firm_mass, survive, transition, install_cost.reshape(1, 128))
    return values, relative.reshape(SEC)


def solution(mesh):
    placed = (
        P("sector", None, "cap"),
        P("sector", None, "cap"),
        P("sector", None, "cap"),
        P("sector"),
        P("sector"),
        P(),
        P("cap"),
    )
    return jax.shard_map(
        on_device,
        mesh=mesh,
        in_specs=placed,
        out_specs=(P("sector", None, "cap"), P("sector")),
        check_vma=False,
    )
```

```python
import math

import jax
import jax.numpy as jnp
import numpy as np
from jax import lax
from jax.experimental import pallas as pl
from jax.experimental.pallas import tpu as pltpu
from jax.sharding import PartitionSpec as P

K = 2048
Z = 32
SWEEPS = 2
SEC = 8
CAPS = 16
REACH = 4
ZS = 16
ROWS = 16
CHUNK = 32
CHUNKS = K // CHUNK
STEPS = CHUNKS + CAPS - 1
SPLIT = 53
GROUPS = K // 8
LINES = GROUPS + 8 * (CAPS - 1)
SHIFT = 8 * (CAPS - 1)
ENDS = 96
NEG = -1e30
LOG10 = float(np.log(np.float32(10.0)))


def capital_of(positions):
    return 0.2 * jnp.exp(LOG10 * positions.astype(jnp.float32) / (K - 1))


def iota(shape, axis):
    return lax.broadcasted_iota(jnp.int32, shape, axis)


def kernel(
    exit_ref, demand_ref, start_hbm, mass_hbm, survive_hbm, trans_hbm, install_hbm,
    value_ref, rel_ref,
    forward, heard, heights, lines, table, jumps, table_s, jumps_s,
    reached, folded, reply, best, part, parts, root, pair, both, near, quad, far,
    mass_ref, survive_ref, trans_ref, install_ref,
    fwd_send, fwd_recv, rep_send, rep_recv, par_send, par_recv, pair_send, pair_recv,
    near_send, near_recv, far_send, far_recv, table_sem, load_sem,
):
    me = lax.axis_index("cap")
    sec = lax.axis_index("sector")
    core = lax.rem(sec, 2)
    level = sec // 2
    partner = sec + 1 - 2 * core

    def cap_at(d):
        return {"cap": lax.rem(me + d, CAPS)}

    def level_at(d):
        return {"sector": 2 * lax.rem(level + d + ZS, ZS) + core}

    barrier = pltpu.get_barrier_semaphore()

    def greet(d, c):
        pl.semaphore_signal(barrier, inc=1, device_id=cap_at(d))
        return c

    loads = [
        pltpu.make_async_copy(source, target, load_sem.at[i])
        for i, (source, target) in enumerate((
            (start_hbm, value_ref), (mass_hbm, mass_ref), (survive_hbm, survive_ref),
            (trans_hbm, trans_ref), (install_hbm, install_ref)))
    ]
    for load in loads:
        load.start()
    lax.fori_loop(1, CAPS, greet, 0)
    for d in range(1, REACH + 1):
        pl.semaphore_signal(barrier, inc=1, device_id=level_at(d))
        pl.semaphore_signal(barrier, inc=1, device_id=level_at(-d))
    pl.semaphore_signal(barrier, inc=1, device_id={"sector": partner})

    capital_all = capital_of(iota((CAPS, 128), 0) * 128 + iota((CAPS, 128), 1))
    half = 0.8 * capital_all
    square_all = capital_all * capital_all
    low = iota((8, 128), 1) % 8
    own_place = 2 * low - 8 * (iota((8, 128), 1) // 8) - iota((8, 128), 0)

    def fill(i, c):
        lines[i] = capital_of(16 * (i - SHIFT) + own_place)
        return c

    lax.fori_loop(0, LINES, fill, 0, unroll=8)
    place = me * 128 + iota((1, 128), 1)
    capital = capital_of(place)
    scrap = 0.3 * capital
    log_cap = math.log(0.2) + LOG10 * place.astype(jnp.float32) / (K - 1)
    log_prod = -0.5 + iota((Z, 128), 0).astype(jnp.float32) / (Z - 1)
    output = jnp.exp(log_prod + 0.6 * log_cap)
    lane = iota((ROWS, 128), 1)
    lane_f = lane.astype(jnp.float32)

    def fwd_copy(sweep, d):
        peer = lax.rem(me + d, CAPS)
        return pltpu.make_async_remote_copy(
            forward.at[sweep, peer], heard.at[sweep, me], fwd_send.at[sweep, d], fwd_recv.at[sweep, d],
            device_id=cap_at(d))

    def rep_copy(sweep, d):
        peer = lax.rem(me + d, CAPS)
        return pltpu.make_async_remote_copy(
            reply.at[sweep, peer], best.at[sweep, me], rep_send.at[sweep, d], rep_recv.at[sweep, d],
            device_id=cap_at(d))

    def par_copy(sweep, d):
        return pltpu.make_async_remote_copy(
            part.at[sweep], parts.at[sweep, me], par_send.at[sweep, d], par_recv.at[sweep, d],
            device_id=cap_at(d))

    def near_copy(sweep, d):
        return pltpu.make_async_remote_copy(
            both.at[sweep], near.at[sweep, d], near_send.at[sweep, d], near_recv.at[sweep, d],
            device_id=level_at(-d))

    def far_copy(sweep, i):
        return pltpu.make_async_remote_copy(
            far.at[sweep, 1] if i == 2 else quad.at[sweep], far.at[sweep, i],
            far_send.at[sweep, i], far_recv.at[sweep, i],
            device_id=level_at(REACH if i == 0 else -REACH))

    def start_all(copy, sweep):
        def one(d, c):
            copy(sweep, d).start()
            return c
        lax.fori_loop(1, CAPS, one, 0)

    def wait_all(copy, sweep):
        def one(d, c):
            copy(sweep, d).wait()
            return c
        lax.fori_loop(1, CAPS, one, 0)

    for load in loads:
        load.wait()
    install = install_ref[...]

    def sweep_body(sweep, carry):
        sums = []
        for s in range(SEC):
            live = (survive_ref[s] == 1) & (iota((Z, 128), 0) >= exit_ref[s])
            values = value_ref[s]
            staying = jnp.where(live, jax.nn.sigmoid((values - scrap) * 2.0), 0.0)
            sums.append(jnp.sum(mass_ref[s] * staying * output, axis=0, keepdims=True))
            continuation = jnp.where(live, jnp.maximum(values, scrap), scrap)
            expect = lax.dot_general(
                trans_ref[...], continuation, (((1,), (0,)), ((), ())),
                precision=lax.Precision.HIGHEST, preferred_element_type=jnp.float32)
            ahead = 0.9 * expect - install
            forward[sweep, 2 * s] = ahead[:ROWS]
            forward[sweep, 2 * s + 1] = ahead[ROWS:]
        part[sweep] = jnp.concatenate(sums, axis=0)

        @pl.when(sweep == 0)
        def _():
            pl.semaphore_wait(barrier, CAPS - 1 + 2 * REACH + 1)

        start_all(par_copy, sweep)
        start_all(fwd_copy, sweep)
        heard[sweep, me] = forward[sweep, me]
        parts[sweep, me] = part[sweep]
        wait_all(par_copy, sweep)
        whole = jnp.sum(jnp.sum(parts[sweep], axis=0), axis=1, keepdims=True)
        supply = 1.0 + jnp.broadcast_to(whole, (SEC, 128)) / (Z * K)
        demand = jnp.zeros((SEC, 128), jnp.float32)
        for s in range(SEC):
            demand = jnp.where(iota((SEC, 128), 0) == s, demand_ref[s], demand)
        prices = jnp.sqrt(demand / supply)
        root[sweep] = jnp.sum(jnp.sqrt(prices), axis=0, keepdims=True)
        to_pair = pltpu.make_async_remote_copy(
            root.at[sweep], pair.at[sweep], pair_send.at[sweep], pair_recv.at[sweep],
            device_id={"sector": partner})
        to_pair.start()

        wait_all(fwd_copy, sweep)
        to_pair.wait()
        both[sweep] = root[sweep] + pair[sweep]
        for d in range(1, REACH):
            near_copy(sweep, d).start()

        def spread(i, c):
            rows = [heard[sweep, i] + 0.8 * capital_of(i * 128 + iota((1, 128), 1))]
            for bit in (64, 32, 16, 8):
                high = (lane // bit) % 2 == 1
                wide = []
                for x in rows:
                    turned = pltpu.roll(x, bit, 1)
                    wide += [jnp.where(high, turned, x), jnp.where(high, x, turned)]
                rows = wide
            for g in range(16):
                heights[16 * i + g] = rows[g]
            return c

        lax.fori_loop(0, CAPS, spread, 0)

        tall = heard[sweep] + half[:, None, :]
        source = lax.broadcasted_iota(jnp.int32, (CAPS, ROWS, 128), 0).astype(jnp.float32)
        chunks = []
        for b in range(1, CAPS):
            rate = 1.0 / (0.2 * math.exp(LOG10 * 128 * b / (K - 1)))
            here = tall - (square_all * rate)[:, None, :]
            top = jnp.max(here, axis=0)
            where = jnp.min(jnp.where(here == top[None], source, 1e9), axis=0)
            peak = jnp.max(top, axis=1, keepdims=True)
            spot = where * (128 // CHUNK) + (lane // CHUNK).astype(jnp.float32)
            chunk = jnp.min(jnp.where(top == peak, spot, 1e9), axis=1, keepdims=True)
            chunk = jnp.broadcast_to(chunk, (ROWS, 128))
            chunks.append(jnp.maximum(chunk, chunks[-1]) if chunks else chunk)
        chunks.append(jnp.full((ROWS, 128), float(CHUNKS - 1), jnp.float32))
        block = jnp.zeros((ROWS, 128), jnp.float32)
        jump = jnp.zeros((ROWS, 128), jnp.float32)
        for b in range(1, CAPS):
            first = chunks[b - 1] + float(b)
            block = block + jnp.where(first <= lane_f, 1.0, 0.0)
            jump = jnp.where(first == lane_f, NEG, jump)
        group = 4.0 * (lane_f - block)
        line = group - 8.0 * block + float(SHIFT)
        for b in range(CAPS):
            group = jnp.where(lane == ENDS + b, chunks[b] + float(b), group)
        table[:ROWS] = jnp.clip(group.astype(jnp.int32), 0, jnp.where(lane < ENDS, GROUPS - 4, STEPS - 1))
        table[ROWS:] = jnp.clip(line.astype(jnp.int32), 0, LINES - 4)
        jumps[...] = jump
        to_table = pltpu.make_async_copy(table, table_s, table_sem.at[0])
        to_jumps = pltpu.make_async_copy(jumps, jumps_s, table_sem.at[1])
        to_table.start()
        to_jumps.start()
        to_table.wait()
        to_jumps.wait()

        def step(t, accs):
            out = []
            for r in range(ROWS):
                at_height = table_s[r, t]
                at_line = table_s[ROWS + r, t]
                value = heights[pl.ds(at_height, 4), r:r + 1, :] - lines[pl.ds(at_line, 4)]
                acc = jnp.maximum(jnp.max(value, axis=0), accs[r] + jumps_s[r, t])
                reached[r, t] = acc
                out.append(acc)
            return tuple(out)

        accs = lax.fori_loop(0, SPLIT, step, tuple(jnp.full((8, 128), NEG, jnp.float32) for _ in range(ROWS)))
        four = both[sweep]
        for d in range(1, REACH):
            near_copy(sweep, d).wait()
            four = four + near[sweep, d]
        quad[sweep] = four
        far_copy(sweep, 0).start()
        far_copy(sweep, 1).start()
        lax.fori_loop(SPLIT, STEPS, step, accs)

        for h in range(2):
            odd = iota((ROWS * 8, 128), 1)
            tops = []
            for p in range(8):
                tops.append(jnp.concatenate(
                    [reached[r, table_s[r, ENDS + 8 * h + p]] for r in range(ROWS)], axis=0))
            for bit in (4, 2, 1):
                high = (odd // bit) % 2 == 1
                less = []
                for i in range(len(tops) // 2):
                    x, y = tops[i], tops[i + len(tops) // 2]
                    mine = jnp.where(high, y, x)
                    other = jnp.where(high, x, y)
                    other = jnp.where(high, pltpu.roll(other, bit, 1), pltpu.roll(other, 128 - bit, 1))
                    less.append(jnp.maximum(mine, other))
                tops = less
            folded[h] = tops[0].reshape(ROWS, 8, 128)
            ways = [folded[h, :, q, :] for q in range(8)]
            for bit in (4, 2, 1):
                high = (lane // bit) % 2 == 1
                for q in range(8):
                    if q & bit == 0:
                        x, y = ways[q], ways[q + bit]
                        ways[q] = jnp.where(high, pltpu.roll(y, bit, 1), x)
                        ways[q + bit] = jnp.where(high, y, pltpu.roll(x, 128 - bit, 1))
            for p in range(8):
                reply[sweep, 8 * h + p] = ways[p]
        start_all(rep_copy, sweep)
        best[sweep, me] = reply[sweep, me]
        far_copy(sweep, 1).wait()
        far_copy(sweep, 2).start()
        far_copy(sweep, 0).wait()
        far_copy(sweep, 2).wait()
        root_sum = quad[sweep] + far[sweep, 0] + far[sweep, 1] + far[sweep, 2]
        price_index = root_sum / (SEC * 2 * ZS)
        price_index = price_index * price_index
        relative = prices / price_index
        wait_all(rep_copy, sweep)
        for s in range(SEC):
            for h in range(2):
                top = best[sweep, 2 * s + h] - 1.41 * capital
                stay = forward[sweep, 2 * s + h] - 0.11 * capital
                gain = jnp.maximum(top, stay)
                rows = slice(h * ROWS, (h + 1) * ROWS)
                live = (survive_ref[s, rows] == 1) & (iota((ROWS, 128), 0) + h * ROWS >= exit_ref[s])
                value_ref[s, rows] = jnp.where(live, relative[s:s + 1] * output[rows] + gain, scrap)
        flat = jnp.where(iota((SEC, 128), 0) == iota((SEC, 128), 1), relative, 0.0)
        rel_ref[...] = jnp.sum(flat, axis=0, keepdims=True)[:, :SEC]
        return carry

    lax.fori_loop(0, SWEEPS, sweep_body, 0)


def on_device(start_value, firm_mass, survive, exit_index, demand, transition, install_cost):
    f32 = jnp.float32
    vmem = pl.BlockSpec(memory_space=pltpu.VMEM)
    smem = pl.BlockSpec(memory_space=pltpu.SMEM)
    dma = pltpu.SemaphoreType.DMA
    values, relative = pl.pallas_call(
        kernel,
        out_shape=(jax.ShapeDtypeStruct((SEC, Z, 128), f32), jax.ShapeDtypeStruct((1, SEC), f32)),
        in_specs=[smem, smem] + [pl.BlockSpec(memory_space=pl.ANY)] * 5,
        out_specs=(vmem, vmem),
        scratch_shapes=[
            pltpu.VMEM((SWEEPS, CAPS, ROWS, 128), f32),
            pltpu.VMEM((SWEEPS, CAPS, ROWS, 128), f32),
            pltpu.VMEM((GROUPS, ROWS, 128), f32),
            pltpu.VMEM((LINES, 8, 128), f32),
            pltpu.VMEM((2 * ROWS, 128), jnp.int32),
            pltpu.VMEM((ROWS, 128), f32),
            pltpu.SMEM((2 * ROWS, 128), jnp.int32),
            pltpu.SMEM((ROWS, 128), f32),
            pltpu.VMEM((ROWS, STEPS, 8, 128), f32),
            pltpu.VMEM((2, ROWS, 8, 128), f32),
            pltpu.VMEM((SWEEPS, CAPS, ROWS, 128), f32),
            pltpu.VMEM((SWEEPS, CAPS, ROWS, 128), f32),
            pltpu.VMEM((SWEEPS, SEC, 128), f32),
            pltpu.VMEM((SWEEPS, CAPS, SEC, 128), f32),
            pltpu.VMEM((SWEEPS, 1, 128), f32),
            pltpu.VMEM((SWEEPS, 1, 128), f32),
            pltpu.VMEM((SWEEPS, 1, 128), f32),
            pltpu.VMEM((SWEEPS, REACH, 1, 128), f32),
            pltpu.VMEM((SWEEPS, 1, 128), f32),
            pltpu.VMEM((SWEEPS, 3, 1, 128), f32),
            pltpu.VMEM((SEC, Z, 128), f32),
            pltpu.VMEM((SEC, Z, 128), jnp.int32),
            pltpu.VMEM((Z, Z), f32),
            pltpu.VMEM((1, 128), f32),
            dma((SWEEPS, CAPS)), dma((SWEEPS, CAPS)), dma((SWEEPS, CAPS)), dma((SWEEPS, CAPS)),
            dma((SWEEPS, CAPS)), dma((SWEEPS, CAPS)), dma((SWEEPS,)), dma((SWEEPS,)),
            dma((SWEEPS, REACH)), dma((SWEEPS, REACH)), dma((SWEEPS, 3)), dma((SWEEPS, 3)), dma((2,)), dma((5,)),
        ],
        compiler_params=pltpu.CompilerParams(
            collective_id=0, has_side_effects=True, vmem_limit_bytes=60 << 20),
    )(exit_index, demand, start_value, firm_mass, survive, transition, install_cost.reshape(1, 128))
    return values, relative.reshape(SEC)


def solution(mesh):
    placed = (
        P("sector", None, "cap"),
        P("sector", None, "cap"),
        P("sector", None, "cap"),
        P("sector"),
        P("sector"),
        P(),
        P("cap"),
    )
    return jax.shard_map(
        on_device,
        mesh=mesh,
        in_specs=placed,
        out_specs=(P("sector", None, "cap"), P("sector")),
        check_vma=False,
    )
```

```python
import math

import jax
import jax.numpy as jnp
import numpy as np
from jax import lax
from jax.experimental import pallas as pl
from jax.experimental.pallas import tpu as pltpu
from jax.sharding import PartitionSpec as P

K = 2048
Z = 32
SWEEPS = 2
SEC = 8
CAPS = 16
ZS = 16
ROWS = 16
CHUNK = 64
CHUNKS = K // CHUNK
GANG = CHUNK // 8
STEPS = CHUNKS + CAPS - 1
RUN = STEPS + 1
ORDER = sorted(range(1, CAPS), key=lambda d: -sum(min(x, 4 - x) for x in (d // 4, d % 4)))
FAR = sorted(range(1, ZS), key=lambda d: -min(d, ZS - d))
GROUPS = K // 8
LINES = GROUPS + 8 * (CAPS - 1)
SHIFT = 8 * (CAPS - 1)
ENDS = 96
NEG = -1e30
LOG10 = float(np.log(np.float32(10.0)))


def capital_of(positions):
    return 0.2 * jnp.exp(LOG10 * positions.astype(jnp.float32) / (K - 1))


def iota(shape, axis):
    return lax.broadcasted_iota(jnp.int32, shape, axis)


def kernel(
    exit_ref, demand_ref, start_hbm, mass_hbm, survive_hbm, trans_hbm, install_hbm,
    value_ref, rel_ref,
    forward, heard, heights, lines, table, jumps, table_s, jumps_s,
    reached, folded, reply, best, part, parts, root, pair, both, roots,
    mass_ref, survive_ref, trans_ref, install_ref,
    fwd_send, fwd_recv, rep_send, rep_recv, par_send, par_recv, pair_send, pair_recv,
    root_send, root_recv, table_sem, load_sem,
):
    me = lax.axis_index("cap")
    sec = lax.axis_index("sector")
    core = lax.rem(sec, 2)
    level = sec // 2
    partner = sec + 1 - 2 * core

    row, column = me // 4, lax.rem(me, 4)

    def peer_of(d):
        return 4 * lax.rem(row + d // 4, 4) + lax.rem(column + d % 4, 4)

    def source_of(d):
        return 4 * lax.rem(row + 4 - d // 4, 4) + lax.rem(column + 4 - d % 4, 4)

    def cap_at(d):
        return {"cap": peer_of(d)}

    def level_at(d):
        return {"sector": 2 * lax.rem(level + d, ZS) + core}

    barrier = pltpu.get_barrier_semaphore()

    for d in ORDER:
        pl.semaphore_signal(barrier, inc=1, device_id=cap_at(d))
    for d in FAR:
        pl.semaphore_signal(barrier, inc=1, device_id=level_at(d))
    pl.semaphore_signal(barrier, inc=1, device_id={"sector": partner})

    loads = [
        pltpu.make_async_copy(source, target, load_sem.at[i])
        for i, (source, target) in enumerate((
            (start_hbm, value_ref), (mass_hbm, mass_ref), (survive_hbm, survive_ref),
            (trans_hbm, trans_ref), (install_hbm, install_ref)))
    ]
    for load in loads:
        load.start()

    capital_all = capital_of(iota((CAPS, 128), 0) * 128 + iota((CAPS, 128), 1))
    half = 0.8 * capital_all
    square_all = capital_all * capital_all
    low = iota((8, 128), 1) % 8
    own_place = 2 * low - 8 * (iota((8, 128), 1) // 8) - iota((8, 128), 0)

    def fill(i, c):
        lines[i] = capital_of(16 * (i - SHIFT) + own_place)
        return c

    lax.fori_loop(0, LINES, fill, 0, unroll=8)
    place = me * 128 + iota((1, 128), 1)
    capital = capital_of(place)
    scrap = 0.3 * capital
    log_cap = math.log(0.2) + LOG10 * place.astype(jnp.float32) / (K - 1)
    log_prod = -0.5 + iota((Z, 128), 0).astype(jnp.float32) / (Z - 1)
    output = jnp.exp(log_prod + 0.6 * log_cap)
    lane = iota((ROWS, 128), 1)
    lane_f = lane.astype(jnp.float32)

    def fwd_copy(sweep, d):
        peer = peer_of(d)
        return pltpu.make_async_remote_copy(
            forward.at[sweep, peer], heard.at[sweep, me], fwd_send.at[sweep, d], fwd_recv.at[sweep, d],
            device_id=cap_at(d))

    def rep_copy(sweep, d):
        peer = peer_of(d)
        return pltpu.make_async_remote_copy(
            reply.at[sweep, peer], best.at[sweep, me], rep_send.at[sweep, d], rep_recv.at[sweep, d],
            device_id=cap_at(d))

    def par_copy(sweep, d):
        return pltpu.make_async_remote_copy(
            part.at[sweep], parts.at[sweep, me], par_send.at[sweep, d], par_recv.at[sweep, d],
            device_id=cap_at(d))

    def root_copy(sweep, d):
        return pltpu.make_async_remote_copy(
            both.at[sweep], roots.at[sweep, level], root_send.at[sweep, d], root_recv.at[sweep, d],
            device_id=level_at(d))

    def start_all(copy, sweep):
        for d in ORDER:
            copy(sweep, d).start()

    def wait_all(copy, sweep):
        for d in ORDER:
            copy(sweep, d).wait()

    for load in loads:
        load.wait()
    install = install_ref[...]

    def sweep_body(sweep, carry):
        sums = []
        for s in range(SEC):
            live = (survive_ref[s] == 1) & (iota((Z, 128), 0) >= exit_ref[s])
            values = value_ref[s]
            staying = jnp.where(live, jax.nn.sigmoid((values - scrap) * 2.0), 0.0)
            sums.append(jnp.sum(mass_ref[s] * staying * output, axis=0, keepdims=True))
            continuation = jnp.where(live, jnp.maximum(values, scrap), scrap)
            expect = lax.dot_general(
                trans_ref[...], continuation, (((1,), (0,)), ((), ())),
                precision=lax.Precision.HIGHEST, preferred_element_type=jnp.float32)
            ahead = 0.9 * expect - install
            forward[sweep, 2 * s] = ahead[:ROWS]
            forward[sweep, 2 * s + 1] = ahead[ROWS:]
        sums = jnp.sum(jnp.concatenate(sums, axis=0), axis=1, keepdims=True)
        diagonal = iota((SEC, 128), 0) == iota((SEC, 128), 1)
        part[sweep] = jnp.sum(jnp.where(diagonal, sums, 0.0), axis=0, keepdims=True)

        @pl.when(sweep == 0)
        def _():
            pl.semaphore_wait(barrier, CAPS - 1 + ZS - 1 + 1)

        start_all(par_copy, sweep)
        start_all(fwd_copy, sweep)
        heard[sweep, me] = forward[sweep, me]
        parts[sweep, me] = part[sweep]
        wait_all(par_copy, sweep)
        whole = jnp.sum(jnp.where(diagonal, jnp.sum(parts[sweep], axis=0), 0.0), axis=1, keepdims=True)
        supply = 1.0 + jnp.broadcast_to(whole, (SEC, 128)) / (Z * K)
        demand = jnp.zeros((SEC, 128), jnp.float32)
        for s in range(SEC):
            demand = jnp.where(iota((SEC, 128), 0) == s, demand_ref[s], demand)
        prices = jnp.sqrt(demand / supply)
        root[sweep] = jnp.sum(jnp.sqrt(prices), axis=0, keepdims=True)
        to_pair = pltpu.make_async_remote_copy(
            root.at[sweep], pair.at[sweep], pair_send.at[sweep], pair_recv.at[sweep],
            device_id={"sector": partner})
        to_pair.start()

        def spread(i):
            rows = [heard[sweep, i] + 0.8 * capital_of(i * 128 + iota((1, 128), 1))]
            for bit in (64, 32, 16, 8):
                high = (lane // bit) % 2 == 1
                wide = []
                for x in rows:
                    turned = pltpu.roll(x, bit, 1)
                    wide += [jnp.where(high, turned, x), jnp.where(high, x, turned)]
                rows = wide
            for g in range(16):
                heights[16 * i + g] = rows[g]

        spread(me)
        for d in ORDER:
            fwd_copy(sweep, d).wait()
            spread(source_of(d))
        to_pair.wait()
        both[sweep] = root[sweep] + pair[sweep]
        for d in FAR:
            root_copy(sweep, d).start()
        roots[sweep, level] = both[sweep]

        tall = heard[sweep] + half[:, None, :]
        source = lax.broadcasted_iota(jnp.int32, (CAPS, ROWS, 128), 0).astype(jnp.float32)
        chunks = []
        for b in range(1, CAPS):
            rate = 1.0 / (0.2 * math.exp(LOG10 * 128 * b / (K - 1)))
            here = tall - (square_all * rate)[:, None, :]
            top = jnp.max(here, axis=0)
            where = jnp.min(jnp.where(here == top[None], source, 1e9), axis=0)
            peak = jnp.max(top, axis=1, keepdims=True)
            spot = where * (128 // CHUNK) + (lane // CHUNK).astype(jnp.float32)
            chunk = jnp.min(jnp.where(top == peak, spot, 1e9), axis=1, keepdims=True)
            chunk = jnp.broadcast_to(chunk, (ROWS, 128))
            chunks.append(jnp.maximum(chunk, chunks[-1]) if chunks else chunk)
        chunks.append(jnp.full((ROWS, 128), float(CHUNKS - 1), jnp.float32))
        block = jnp.zeros((ROWS, 128), jnp.float32)
        jump = jnp.zeros((ROWS, 128), jnp.float32)
        for b in range(1, CAPS):
            first = chunks[b - 1] + float(b)
            block = block + jnp.where(first <= lane_f, 1.0, 0.0)
            jump = jnp.where(first == lane_f, NEG, jump)
        group = float(GANG) * (lane_f - block)
        line = group - 8.0 * block + float(SHIFT)
        for b in range(CAPS):
            group = jnp.where(lane == ENDS + b, chunks[b] + float(b), group)
        table[:ROWS] = jnp.clip(group.astype(jnp.int32), 0, jnp.where(lane < ENDS, GROUPS - GANG, STEPS - 1))
        table[ROWS:] = jnp.clip(line.astype(jnp.int32), 0, LINES - GANG)
        jumps[...] = jump
        to_table = pltpu.make_async_copy(table, table_s, table_sem.at[0])
        to_jumps = pltpu.make_async_copy(jumps, jumps_s, table_sem.at[1])
        to_table.start()
        to_jumps.start()
        to_table.wait()
        to_jumps.wait()

        def step(t, accs):
            out = []
            for r in range(ROWS):
                value = heights[pl.ds(table_s[r, t], GANG), r:r + 1, :] - lines[pl.ds(table_s[ROWS + r, t], GANG)]
                acc = jnp.maximum(jnp.max(value, axis=0), accs[r] + jumps_s[r, t])
                reached[r, t] = acc
                out.append(acc)
            return tuple(out)

        accs = tuple(jnp.full((8, 128), NEG, jnp.float32) for _ in range(ROWS))
        lax.fori_loop(0, RUN, step, accs, unroll=2)

        for h in range(2):
            odd = iota((ROWS * 8, 128), 1)
            tops = []
            for p in range(8):
                tops.append(jnp.concatenate(
                    [reached[r, table_s[r, ENDS + 8 * h + p]] for r in range(ROWS)], axis=0))
            for bit in (4, 2, 1):
                high = (odd // bit) % 2 == 1
                less = []
                for i in range(len(tops) // 2):
                    x, y = tops[i], tops[i + len(tops) // 2]
                    mine = jnp.where(high, y, x)
                    other = jnp.where(high, x, y)
                    other = jnp.where(high, pltpu.roll(other, bit, 1), pltpu.roll(other, 128 - bit, 1))
                    less.append(jnp.maximum(mine, other))
                tops = less
            folded[h] = tops[0].reshape(ROWS, 8, 128)
            ways = [folded[h, :, q, :] for q in range(8)]
            for bit in (4, 2, 1):
                high = (lane // bit) % 2 == 1
                for q in range(8):
                    if q & bit == 0:
                        x, y = ways[q], ways[q + bit]
                        ways[q] = jnp.where(high, pltpu.roll(y, bit, 1), x)
                        ways[q + bit] = jnp.where(high, y, pltpu.roll(x, 128 - bit, 1))
            for p in range(8):
                reply[sweep, 8 * h + p] = ways[p]
        start_all(rep_copy, sweep)
        best[sweep, me] = reply[sweep, me]
        for d in FAR:
            root_copy(sweep, d).wait()
        root_sum = jnp.sum(roots[sweep], axis=0)
        price_index = root_sum / (SEC * 2 * ZS)
        price_index = price_index * price_index
        relative = prices / price_index
        wait_all(rep_copy, sweep)
        for s in range(SEC):
            for h in range(2):
                top = best[sweep, 2 * s + h] - 1.41 * capital
                stay = forward[sweep, 2 * s + h] - 0.11 * capital
                gain = jnp.maximum(top, stay)
                rows = slice(h * ROWS, (h + 1) * ROWS)
                live = (survive_ref[s, rows] == 1) & (iota((ROWS, 128), 0) + h * ROWS >= exit_ref[s])
                value_ref[s, rows] = jnp.where(live, relative[s:s + 1] * output[rows] + gain, scrap)
        flat = jnp.where(diagonal, relative, 0.0)
        rel_ref[...] = jnp.sum(flat, axis=0, keepdims=True)[:, :SEC]
        return carry

    lax.fori_loop(0, SWEEPS, sweep_body, 0)


def on_device(start_value, firm_mass, survive, exit_index, demand, transition, install_cost):
    f32 = jnp.float32
    vmem = pl.BlockSpec(memory_space=pltpu.VMEM)
    smem = pl.BlockSpec(memory_space=pltpu.SMEM)
    dma = pltpu.SemaphoreType.DMA
    values, relative = pl.pallas_call(
        kernel,
        out_shape=(jax.ShapeDtypeStruct((SEC, Z, 128), f32), jax.ShapeDtypeStruct((1, SEC), f32)),
        in_specs=[smem, smem] + [pl.BlockSpec(memory_space=pl.ANY)] * 5,
        out_specs=(vmem, vmem),
        scratch_shapes=[
            pltpu.VMEM((SWEEPS, CAPS, ROWS, 128), f32),
            pltpu.VMEM((SWEEPS, CAPS, ROWS, 128), f32),
            pltpu.VMEM((GROUPS, ROWS, 128), f32),
            pltpu.VMEM((LINES, 8, 128), f32),
            pltpu.VMEM((2 * ROWS, 128), jnp.int32),
            pltpu.VMEM((ROWS, 128), f32),
            pltpu.SMEM((2 * ROWS, 128), jnp.int32),
            pltpu.SMEM((ROWS, 128), f32),
            pltpu.VMEM((ROWS, RUN, 8, 128), f32),
            pltpu.VMEM((2, ROWS, 8, 128), f32),
            pltpu.VMEM((SWEEPS, CAPS, ROWS, 128), f32),
            pltpu.VMEM((SWEEPS, CAPS, ROWS, 128), f32),
            pltpu.VMEM((SWEEPS, 1, 128), f32),
            pltpu.VMEM((SWEEPS, CAPS, 1, 128), f32),
            pltpu.VMEM((SWEEPS, 1, 128), f32),
            pltpu.VMEM((SWEEPS, 1, 128), f32),
            pltpu.VMEM((SWEEPS, 1, 128), f32),
            pltpu.VMEM((SWEEPS, ZS, 1, 128), f32),
            pltpu.VMEM((SEC, Z, 128), f32),
            pltpu.VMEM((SEC, Z, 128), jnp.int32),
            pltpu.VMEM((Z, Z), f32),
            pltpu.VMEM((1, 128), f32),
            dma((SWEEPS, CAPS)), dma((SWEEPS, CAPS)), dma((SWEEPS, CAPS)), dma((SWEEPS, CAPS)),
            dma((SWEEPS, CAPS)), dma((SWEEPS, CAPS)), dma((SWEEPS,)), dma((SWEEPS,)),
            dma((SWEEPS, ZS)), dma((SWEEPS, ZS)), dma((2,)), dma((5,)),
        ],
        compiler_params=pltpu.CompilerParams(
            collective_id=0, has_side_effects=True, vmem_limit_bytes=60 << 20),
    )(exit_index, demand, start_value, firm_mass, survive, transition, install_cost.reshape(1, 128))
    return values, relative.reshape(SEC)


def solution(mesh):
    placed = (
        P("sector", None, "cap"),
        P("sector", None, "cap"),
        P("sector", None, "cap"),
        P("sector"),
        P("sector"),
        P(),
        P("cap"),
    )
    return jax.shard_map(
        on_device,
        mesh=mesh,
        in_specs=placed,
        out_specs=(P("sector", None, "cap"), P("sector")),
        check_vma=False,
    )
```

```python
import math

import jax
import jax.numpy as jnp
import numpy as np
from jax import lax
from jax.experimental import pallas as pl
from jax.experimental.pallas import tpu as pltpu
from jax.sharding import PartitionSpec as P

K = 2048
Z = 32
SWEEPS = 2
SEC = 8
CAPS = 16
ZS = 16
ROWS = 16
CHUNK = 64
CHUNKS = K // CHUNK
GANG = CHUNK // 8
STEPS = CHUNKS + CAPS - 1
RUN = STEPS + 1
ORDER = sorted(range(1, CAPS), key=lambda d: -sum(min(x, 4 - x) for x in (d // 4, d % 4)))
LATE = ORDER[7:]
FAR = sorted(range(1, ZS), key=lambda d: -min(d, ZS - d))
GROUPS = K // 8
LINES = GROUPS + 8 * (CAPS - 1)
SHIFT = 8 * (CAPS - 1)
ENDS = 96
NEG = -1e30
LOG10 = float(np.log(np.float32(10.0)))


def capital_of(positions):
    return 0.2 * jnp.exp(LOG10 * positions.astype(jnp.float32) / (K - 1))


def iota(shape, axis):
    return lax.broadcasted_iota(jnp.int32, shape, axis)


def kernel(
    exit_ref, demand_ref, start_hbm, mass_hbm, survive_hbm, trans_hbm, install_hbm,
    value_ref, rel_ref,
    forward, heard, heights, lines, table, jumps, table_s, jumps_s,
    reached, folded, reply, best, part, parts, root, pair, both, roots,
    mass_ref, survive_ref, trans_ref, install_ref,
    fwd_send, fwd_recv, rep_send, rep_recv, par_send, par_recv, pair_send, pair_recv,
    root_send, root_recv, table_sem, load_sem,
):
    me = lax.axis_index("cap")
    sec = lax.axis_index("sector")
    core = lax.rem(sec, 2)
    level = sec // 2
    partner = sec + 1 - 2 * core

    row, column = me // 4, lax.rem(me, 4)

    def peer_of(d):
        return 4 * lax.rem(row + d // 4, 4) + lax.rem(column + d % 4, 4)

    def source_of(d):
        return 4 * lax.rem(row + 4 - d // 4, 4) + lax.rem(column + 4 - d % 4, 4)

    def cap_at(d):
        return {"cap": peer_of(d)}

    def level_at(d):
        return {"sector": 2 * lax.rem(level + d, ZS) + core}

    barrier = pltpu.get_barrier_semaphore()

    for d in ORDER:
        pl.semaphore_signal(barrier, inc=1, device_id=cap_at(d))
    for d in FAR:
        pl.semaphore_signal(barrier, inc=1, device_id=level_at(d))
    pl.semaphore_signal(barrier, inc=1, device_id={"sector": partner})

    loads = [
        pltpu.make_async_copy(source, target, load_sem.at[i])
        for i, (source, target) in enumerate((
            (start_hbm, value_ref), (mass_hbm, mass_ref), (survive_hbm, survive_ref),
            (trans_hbm, trans_ref), (install_hbm, install_ref)))
    ]
    for load in loads:
        load.start()

    capital_all = capital_of(iota((CAPS, 128), 0) * 128 + iota((CAPS, 128), 1))
    half = 0.8 * capital_all
    square_all = capital_all * capital_all
    low = iota((8, 128), 1) % 8
    own_place = 2 * low - 8 * (iota((8, 128), 1) // 8) - iota((8, 128), 0)

    def fill(i, c):
        lines[i] = capital_of(16 * (i - SHIFT) + own_place)
        return c

    lax.fori_loop(0, LINES, fill, 0, unroll=8)
    place = me * 128 + iota((1, 128), 1)
    capital = capital_of(place)
    scrap = 0.3 * capital
    log_cap = math.log(0.2) + LOG10 * place.astype(jnp.float32) / (K - 1)
    log_prod = -0.5 + iota((Z, 128), 0).astype(jnp.float32) / (Z - 1)
    output = jnp.exp(log_prod + 0.6 * log_cap)
    lane = iota((ROWS, 128), 1)
    lane_f = lane.astype(jnp.float32)

    def fwd_copy(sweep, d):
        peer = peer_of(d)
        return pltpu.make_async_remote_copy(
            forward.at[sweep, peer], heard.at[sweep, me], fwd_send.at[sweep, d], fwd_recv.at[sweep, d],
            device_id=cap_at(d))

    def rep_copy(sweep, d):
        peer = peer_of(d)
        return pltpu.make_async_remote_copy(
            reply.at[sweep, peer], best.at[sweep, me], rep_send.at[sweep, d], rep_recv.at[sweep, d],
            device_id=cap_at(d))

    def par_copy(sweep, d):
        return pltpu.make_async_remote_copy(
            part.at[sweep], parts.at[sweep, me], par_send.at[sweep, d], par_recv.at[sweep, d],
            device_id=cap_at(d))

    def root_copy(sweep, d):
        return pltpu.make_async_remote_copy(
            both.at[sweep], roots.at[sweep, level], root_send.at[sweep, d], root_recv.at[sweep, d],
            device_id=level_at(d))

    def start_all(copy, sweep):
        for d in ORDER:
            copy(sweep, d).start()

    def wait_all(copy, sweep):
        for d in ORDER:
            copy(sweep, d).wait()

    for load in loads:
        load.wait()
    install = install_ref[...]

    def sweep_body(sweep, carry):
        sums = []
        for s in range(SEC):
            live = (survive_ref[s] == 1) & (iota((Z, 128), 0) >= exit_ref[s])
            values = value_ref[s]
            staying = jnp.where(live, jax.nn.sigmoid((values - scrap) * 2.0), 0.0)
            sums.append(jnp.sum(mass_ref[s] * staying * output, axis=0, keepdims=True))
            continuation = jnp.where(live, jnp.maximum(values, scrap), scrap)
            expect = lax.dot_general(
                trans_ref[...], continuation, (((1,), (0,)), ((), ())),
                precision=lax.Precision.HIGHEST, preferred_element_type=jnp.float32)
            ahead = 0.9 * expect - install
            forward[sweep, 2 * s] = ahead[:ROWS]
            forward[sweep, 2 * s + 1] = ahead[ROWS:]
        sums = jnp.sum(jnp.concatenate(sums, axis=0), axis=1, keepdims=True)
        diagonal = iota((SEC, 128), 0) == iota((SEC, 128), 1)
        part[sweep] = jnp.sum(jnp.where(diagonal, sums, 0.0), axis=0, keepdims=True)

        @pl.when(sweep == 0)
        def _():
            pl.semaphore_wait(barrier, CAPS - 1 + ZS - 1 + 1)

        start_all(par_copy, sweep)
        start_all(fwd_copy, sweep)
        heard[sweep, me] = forward[sweep, me]
        parts[sweep, me] = part[sweep]
        wait_all(par_copy, sweep)
        whole = jnp.sum(jnp.where(diagonal, jnp.sum(parts[sweep], axis=0), 0.0), axis=1, keepdims=True)
        supply = 1.0 + jnp.broadcast_to(whole, (SEC, 128)) / (Z * K)
        demand = jnp.zeros((SEC, 128), jnp.float32)
        for s in range(SEC):
            demand = jnp.where(iota((SEC, 128), 0) == s, demand_ref[s], demand)
        prices = jnp.sqrt(demand / supply)
        root[sweep] = jnp.sum(jnp.sqrt(prices), axis=0, keepdims=True)
        to_pair = pltpu.make_async_remote_copy(
            root.at[sweep], pair.at[sweep], pair_send.at[sweep], pair_recv.at[sweep],
            device_id={"sector": partner})
        to_pair.start()

        def spread(i):
            rows = [heard[sweep, i] + 0.8 * capital_of(i * 128 + iota((1, 128), 1))]
            for bit in (64, 32, 16, 8):
                high = (lane // bit) % 2 == 1
                wide = []
                for x in rows:
                    turned = pltpu.roll(x, bit, 1)
                    wide += [jnp.where(high, turned, x), jnp.where(high, x, turned)]
                rows = wide
            for g in range(16):
                heights[16 * i + g] = rows[g]

        spread(me)
        for d in ORDER:
            fwd_copy(sweep, d).wait()
            if d not in LATE:
                spread(source_of(d))
        to_pair.wait()
        both[sweep] = root[sweep] + pair[sweep]
        for d in FAR:
            root_copy(sweep, d).start()
        roots[sweep, level] = both[sweep]

        tall = heard[sweep] + half[:, None, :]
        source = lax.broadcasted_iota(jnp.int32, (CAPS, ROWS, 128), 0).astype(jnp.float32)
        chunks = []
        for b in range(1, CAPS):
            rate = 1.0 / (0.2 * math.exp(LOG10 * 128 * b / (K - 1)))
            here = tall - (square_all * rate)[:, None, :]
            top = jnp.max(here, axis=0)
            where = jnp.min(jnp.where(here == top[None], source, 1e9), axis=0)
            peak = jnp.max(top, axis=1, keepdims=True)
            spot = where * (128 // CHUNK) + (lane // CHUNK).astype(jnp.float32)
            chunk = jnp.min(jnp.where(top == peak, spot, 1e9), axis=1, keepdims=True)
            chunk = jnp.broadcast_to(chunk, (ROWS, 128))
            chunks.append(jnp.maximum(chunk, chunks[-1]) if chunks else chunk)
        chunks.append(jnp.full((ROWS, 128), float(CHUNKS - 1), jnp.float32))
        block = jnp.zeros((ROWS, 128), jnp.float32)
        jump = jnp.zeros((ROWS, 128), jnp.float32)
        for b in range(1, CAPS):
            first = chunks[b - 1] + float(b)
            block = block + jnp.where(first <= lane_f, 1.0, 0.0)
            jump = jnp.where(first == lane_f, NEG, jump)
        group = float(GANG) * (lane_f - block)
        line = group - 8.0 * block + float(SHIFT)
        for b in range(CAPS):
            group = jnp.where(lane == ENDS + b, chunks[b] + float(b), group)
        table[:ROWS] = jnp.clip(group.astype(jnp.int32), 0, jnp.where(lane < ENDS, GROUPS - GANG, STEPS - 1))
        table[ROWS:] = jnp.clip(line.astype(jnp.int32), 0, LINES - GANG)
        jumps[...] = jump
        to_table = pltpu.make_async_copy(table, table_s, table_sem.at[0])
        to_jumps = pltpu.make_async_copy(jumps, jumps_s, table_sem.at[1])
        to_table.start()
        to_jumps.start()
        for d in LATE:
            spread(source_of(d))
        to_table.wait()
        to_jumps.wait()

        def step(t, accs):
            out = []
            for r in range(ROWS):
                value = heights[pl.ds(table_s[r, t], GANG), r:r + 1, :] - lines[pl.ds(table_s[ROWS + r, t], GANG)]
                acc = jnp.maximum(jnp.max(value, axis=0), accs[r] + jumps_s[r, t])
                reached[r, t] = acc
                out.append(acc)
            return tuple(out)

        accs = tuple(jnp.full((8, 128), NEG, jnp.float32) for _ in range(ROWS))
        lax.fori_loop(0, RUN, step, accs, unroll=2)

        for h in (1, 0):
            odd = iota((ROWS * 8, 128), 1)
            tops = []
            group = range(8 * h, 8 * h + 8)
            for d in group:
                tops.append(jnp.concatenate(
                    [reached[r, table_s[r, ENDS + peer_of(d)]] for r in range(ROWS)], axis=0))
            for bit in (4, 2, 1):
                high = (odd // bit) % 2 == 1
                less = []
                for i in range(len(tops) // 2):
                    x, y = tops[i], tops[i + len(tops) // 2]
                    mine = jnp.where(high, y, x)
                    other = jnp.where(high, x, y)
                    other = jnp.where(high, pltpu.roll(other, bit, 1), pltpu.roll(other, 128 - bit, 1))
                    less.append(jnp.maximum(mine, other))
                tops = less
            folded[h] = tops[0].reshape(ROWS, 8, 128)
            ways = [folded[h, :, q, :] for q in range(8)]
            for bit in (4, 2, 1):
                high = (lane // bit) % 2 == 1
                for q in range(8):
                    if q & bit == 0:
                        x, y = ways[q], ways[q + bit]
                        ways[q] = jnp.where(high, pltpu.roll(y, bit, 1), x)
                        ways[q + bit] = jnp.where(high, y, pltpu.roll(x, 128 - bit, 1))
            for p, d in enumerate(group):
                reply[sweep, peer_of(d)] = ways[p]
            for d in ORDER:
                if d in group:
                    rep_copy(sweep, d).start()
        best[sweep, me] = reply[sweep, me]
        for d in FAR:
            root_copy(sweep, d).wait()
        root_sum = jnp.sum(roots[sweep], axis=0)
        price_index = root_sum / (SEC * 2 * ZS)
        price_index = price_index * price_index
        relative = prices / price_index
        wait_all(rep_copy, sweep)
        for s in range(SEC):
            for h in range(2):
                top = best[sweep, 2 * s + h] - 1.41 * capital
                stay = forward[sweep, 2 * s + h] - 0.11 * capital
                gain = jnp.maximum(top, stay)
                rows = slice(h * ROWS, (h + 1) * ROWS)
                live = (survive_ref[s, rows] == 1) & (iota((ROWS, 128), 0) + h * ROWS >= exit_ref[s])
                value_ref[s, rows] = jnp.where(live, relative[s:s + 1] * output[rows] + gain, scrap)
        flat = jnp.where(diagonal, relative, 0.0)
        rel_ref[...] = jnp.sum(flat, axis=0, keepdims=True)[:, :SEC]
        return carry

    lax.fori_loop(0, SWEEPS, sweep_body, 0)


def on_device(start_value, firm_mass, survive, exit_index, demand, transition, install_cost):
    f32 = jnp.float32
    vmem = pl.BlockSpec(memory_space=pltpu.VMEM)
    smem = pl.BlockSpec(memory_space=pltpu.SMEM)
    dma = pltpu.SemaphoreType.DMA
    values, relative = pl.pallas_call(
        kernel,
        out_shape=(jax.ShapeDtypeStruct((SEC, Z, 128), f32), jax.ShapeDtypeStruct((1, SEC), f32)),
        in_specs=[smem, smem] + [pl.BlockSpec(memory_space=pltpu.HBM)] * 5,
        out_specs=(vmem, vmem),
        scratch_shapes=[
            pltpu.VMEM((SWEEPS, CAPS, ROWS, 128), f32),
            pltpu.VMEM((SWEEPS, CAPS, ROWS, 128), f32),
            pltpu.VMEM((GROUPS, ROWS, 128), f32),
            pltpu.VMEM((LINES, 8, 128), f32),
            pltpu.VMEM((2 * ROWS, 128), jnp.int32),
            pltpu.VMEM((ROWS, 128), f32),
            pltpu.SMEM((2 * ROWS, 128), jnp.int32),
            pltpu.SMEM((ROWS, 128), f32),
            pltpu.VMEM((ROWS, RUN, 8, 128), f32),
            pltpu.VMEM((2, ROWS, 8, 128), f32),
            pltpu.VMEM((SWEEPS, CAPS, ROWS, 128), f32),
            pltpu.VMEM((SWEEPS, CAPS, ROWS, 128), f32),
            pltpu.VMEM((SWEEPS, 1, 128), f32),
            pltpu.VMEM((SWEEPS, CAPS, 1, 128), f32),
            pltpu.VMEM((SWEEPS, 1, 128), f32),
            pltpu.VMEM((SWEEPS, 1, 128), f32),
            pltpu.VMEM((SWEEPS, 1, 128), f32),
            pltpu.VMEM((SWEEPS, ZS, 1, 128), f32),
            pltpu.VMEM((SEC, Z, 128), f32),
            pltpu.VMEM((SEC, Z, 128), jnp.int32),
            pltpu.VMEM((Z, Z), f32),
            pltpu.VMEM((1, 128), f32),
            dma((SWEEPS, CAPS)), dma((SWEEPS, CAPS)), dma((SWEEPS, CAPS)), dma((SWEEPS, CAPS)),
            dma((SWEEPS, CAPS)), dma((SWEEPS, CAPS)), dma((SWEEPS,)), dma((SWEEPS,)),
            dma((SWEEPS, ZS)), dma((SWEEPS, ZS)), dma((2,)), dma((5,)),
        ],
        compiler_params=pltpu.CompilerParams(
            collective_id=0, has_side_effects=True, vmem_limit_bytes=(40 << 20)),
    )(exit_index, demand, *(pltpu.with_memory_space_constraint(x, pltpu.HBM) for x in (start_value, firm_mass, survive, transition, install_cost.reshape(1, 128))))
    return values, relative.reshape(SEC)


def solution(mesh):
    placed = (
        P("sector", None, "cap"),
        P("sector", None, "cap"),
        P("sector", None, "cap"),
        P("sector"),
        P("sector"),
        P(),
        P("cap"),
    )
    return jax.shard_map(
        on_device,
        mesh=mesh,
        in_specs=placed,
        out_specs=(P("sector", None, "cap"), P("sector")),
        check_vma=False,
    )
```

```python
import math

import jax
import jax.numpy as jnp
import numpy as np
from jax import lax
from jax.experimental import pallas as pl
from jax.experimental.pallas import tpu as pltpu
from jax.sharding import PartitionSpec as P

K = 2048
Z = 32
SWEEPS = 2
SEC = 8
CAPS = 16
ZS = 16
ROWS = 16
CHUNK = 64
CHUNKS = K // CHUNK
GANG = CHUNK // 8
STEPS = CHUNKS + CAPS - 1
RUN = STEPS + 1
ORDER = sorted(range(1, CAPS), key=lambda d: -sum(min(x, 4 - x) for x in (d // 4, d % 4)))
FAR = sorted(range(1, ZS), key=lambda d: -min(d, ZS - d))
GROUPS = K // 8
LINES = GROUPS + 8 * (CAPS - 1)
SHIFT = 8 * (CAPS - 1)
ENDS = 48
LINE_AT = 64
NEG = -1e30
LOG10 = float(np.log(np.float32(10.0)))


def capital_of(positions):
    return 0.2 * jnp.exp(LOG10 * positions.astype(jnp.float32) / (K - 1))


def iota(shape, axis):
    return lax.broadcasted_iota(jnp.int32, shape, axis)


def kernel(
    exit_ref, demand_ref, start_hbm, mass_hbm, survive_hbm, trans_hbm, install_hbm,
    value_ref, rel_ref,
    forward, heard, heights, lines, table, jumps, table_s, jumps_s,
    reached, folded, reply, best, part, parts, root, pair, both, roots,
    mass_ref, survive_ref, trans_ref, install_ref,
    fwd_send, fwd_recv, rep_send, rep_recv, par_send, par_recv, pair_send, pair_recv,
    root_send, root_recv, table_sem, load_sem,
):
    me = lax.axis_index("cap")
    sec = lax.axis_index("sector")
    core = lax.rem(sec, 2)
    level = sec // 2
    partner = sec + 1 - 2 * core

    row, column = me // 4, lax.rem(me, 4)

    def peer_of(d):
        return 4 * lax.rem(row + d // 4, 4) + lax.rem(column + d % 4, 4)

    def source_of(d):
        return 4 * lax.rem(row + 4 - d // 4, 4) + lax.rem(column + 4 - d % 4, 4)

    def cap_at(d):
        return {"cap": peer_of(d)}

    def level_at(d):
        return {"sector": 2 * lax.rem(level + d, ZS) + core}

    barrier = pltpu.get_barrier_semaphore()

    for d in ORDER:
        pl.semaphore_signal(barrier, inc=1, device_id=cap_at(d))
    for d in FAR:
        pl.semaphore_signal(barrier, inc=1, device_id=level_at(d))
    pl.semaphore_signal(barrier, inc=1, device_id={"sector": partner})

    loads = [
        pltpu.make_async_copy(source, target, load_sem.at[i])
        for i, (source, target) in enumerate((
            (start_hbm, value_ref), (mass_hbm, mass_ref), (survive_hbm, survive_ref),
            (trans_hbm, trans_ref), (install_hbm, install_ref)))
    ]
    for load in loads:
        load.start()

    capital_all = capital_of(iota((CAPS, 128), 0) * 128 + iota((CAPS, 128), 1))
    half = 0.8 * capital_all
    square_all = capital_all * capital_all
    low = iota((8, 128), 1) % 8
    own_place = 2 * low - 8 * (iota((8, 128), 1) // 8) - iota((8, 128), 0)

    def fill(i, c):
        lines[i] = capital_of(16 * (i - SHIFT) + own_place)
        return c

    lax.fori_loop(0, LINES, fill, 0, unroll=8)
    place = me * 128 + iota((1, 128), 1)
    capital = capital_of(place)
    scrap = 0.3 * capital
    log_cap = math.log(0.2) + LOG10 * place.astype(jnp.float32) / (K - 1)
    log_prod = -0.5 + iota((Z, 128), 0).astype(jnp.float32) / (Z - 1)
    output = jnp.exp(log_prod + 0.6 * log_cap)
    lane = iota((ROWS, 128), 1)
    lane_f = lane.astype(jnp.float32)

    def fwd_copy(sweep, d):
        peer = peer_of(d)
        return pltpu.make_async_remote_copy(
            forward.at[sweep, peer], heard.at[sweep, me], fwd_send.at[sweep, d], fwd_recv.at[sweep, d],
            device_id=cap_at(d))

    def rep_copy(sweep, d):
        peer = peer_of(d)
        return pltpu.make_async_remote_copy(
            reply.at[sweep, peer], best.at[sweep, me], rep_send.at[sweep, d], rep_recv.at[sweep, d],
            device_id=cap_at(d))

    def par_copy(sweep, d):
        return pltpu.make_async_remote_copy(
            part.at[sweep], parts.at[sweep, me], par_send.at[sweep, d], par_recv.at[sweep, d],
            device_id=cap_at(d))

    def root_copy(sweep, d):
        return pltpu.make_async_remote_copy(
            both.at[sweep], roots.at[sweep, level], root_send.at[sweep, d], root_recv.at[sweep, d],
            device_id=level_at(d))

    def start_all(copy, sweep):
        for d in ORDER:
            copy(sweep, d).start()

    def wait_all(copy, sweep):
        for d in ORDER:
            copy(sweep, d).wait()

    for load in loads:
        load.wait()
    install = install_ref[...]

    def sweep_body(sweep, carry):
        sums = []
        for s in range(SEC):
            live = (survive_ref[s] == 1) & (iota((Z, 128), 0) >= exit_ref[s])
            values = value_ref[s]
            staying = jnp.where(live, jax.nn.sigmoid((values - scrap) * 2.0), 0.0)
            sums.append(jnp.sum(mass_ref[s] * staying * output, axis=0, keepdims=True))
            continuation = jnp.where(live, jnp.maximum(values, scrap), scrap)
            expect = lax.dot_general(
                trans_ref[...], continuation, (((1,), (0,)), ((), ())),
                precision=lax.Precision.HIGHEST, preferred_element_type=jnp.float32)
            ahead = 0.9 * expect - install
            forward[sweep, 2 * s] = ahead[:ROWS]
            forward[sweep, 2 * s + 1] = ahead[ROWS:]
        sums = jnp.sum(jnp.concatenate(sums, axis=0), axis=1, keepdims=True)
        diagonal = iota((SEC, 128), 0) == iota((SEC, 128), 1)
        part[sweep] = jnp.sum(jnp.where(diagonal, sums, 0.0), axis=0, keepdims=True)

        @pl.when(sweep == 0)
        def _():
            pl.semaphore_wait(barrier, CAPS - 1 + ZS - 1 + 1)

        start_all(par_copy, sweep)
        start_all(fwd_copy, sweep)
        heard[sweep, me] = forward[sweep, me]
        parts[sweep, me] = part[sweep]
        wait_all(par_copy, sweep)
        whole = jnp.sum(jnp.where(diagonal, jnp.sum(parts[sweep], axis=0), 0.0), axis=1, keepdims=True)
        supply = 1.0 + jnp.broadcast_to(whole, (SEC, 128)) / (Z * K)
        demand = jnp.zeros((SEC, 128), jnp.float32)
        for s in range(SEC):
            demand = jnp.where(iota((SEC, 128), 0) == s, demand_ref[s], demand)
        prices = jnp.sqrt(demand / supply)
        root[sweep] = jnp.sum(jnp.sqrt(prices), axis=0, keepdims=True)
        to_pair = pltpu.make_async_remote_copy(
            root.at[sweep], pair.at[sweep], pair_send.at[sweep], pair_recv.at[sweep],
            device_id={"sector": partner})
        to_pair.start()

        def spread(i):
            rows = [heard[sweep, i] + 0.8 * capital_of(i * 128 + iota((1, 128), 1))]
            for bit in (64, 32, 16, 8):
                high = (lane // bit) % 2 == 1
                wide = []
                for x in rows:
                    turned = pltpu.roll(x, bit, 1)
                    wide += [jnp.where(high, turned, x), jnp.where(high, x, turned)]
                rows = wide
            for g in range(16):
                heights[16 * i + g] = rows[g]

        wait_all(fwd_copy, sweep)
        to_pair.wait()
        both[sweep] = root[sweep] + pair[sweep]

        tall = heard[sweep] + half[:, None, :]
        source = lax.broadcasted_iota(jnp.int32, (CAPS, ROWS, 128), 0).astype(jnp.float32)
        chunks = []
        for b in range(1, CAPS):
            rate = 1.0 / (0.2 * math.exp(LOG10 * 128 * b / (K - 1)))
            here = tall - (square_all * rate)[:, None, :]
            top = jnp.max(here, axis=0)
            where = jnp.min(jnp.where(here == top[None], source, 1e9), axis=0)
            peak = jnp.max(top, axis=1, keepdims=True)
            spot = where * (128 // CHUNK) + (lane // CHUNK).astype(jnp.float32)
            chunk = jnp.min(jnp.where(top == peak, spot, 1e9), axis=1, keepdims=True)
            chunk = jnp.broadcast_to(chunk, (ROWS, 128))
            chunks.append(jnp.maximum(chunk, chunks[-1]) if chunks else chunk)
        chunks.append(jnp.full((ROWS, 128), float(CHUNKS - 1), jnp.float32))
        block = jnp.zeros((ROWS, 128), jnp.float32)
        jump = jnp.zeros((ROWS, 128), jnp.float32)
        time = lane_f - jnp.where(lane < LINE_AT, 0.0, float(LINE_AT))
        for b in range(1, CAPS):
            first = chunks[b - 1] + float(b)
            block = block + jnp.where(first <= time, 1.0, 0.0)
            jump = jnp.where(first == time, NEG, jump)
        entry = float(GANG) * (time - block)
        entry = entry + jnp.where(lane < LINE_AT, 0.0, float(SHIFT) - 8.0 * block)
        for b in range(CAPS):
            entry = jnp.where(lane == ENDS + b, chunks[b] + float(b), entry)
        limit = jnp.where(lane < ENDS, GROUPS - GANG, jnp.where(lane < LINE_AT, STEPS - 1, LINES - GANG))
        table[...] = jnp.clip(entry.astype(jnp.int32), 0, limit)
        jumps[...] = jump
        to_table = pltpu.make_async_copy(table, table_s, table_sem.at[0])
        to_jumps = pltpu.make_async_copy(jumps, jumps_s, table_sem.at[1])
        to_table.start()
        to_jumps.start()
        for d in FAR:
            root_copy(sweep, d).start()
        roots[sweep, level] = both[sweep]
        spread(me)
        for d in ORDER:
            spread(source_of(d))
        to_table.wait()
        to_jumps.wait()

        def step(t, accs):
            out = []
            for r in range(ROWS):
                value = heights[pl.ds(table_s[r, t], GANG), r:r + 1, :] - lines[pl.ds(table_s[r, LINE_AT + t], GANG)]
                acc = jnp.maximum(jnp.max(value, axis=0), accs[r] + jumps_s[r, t])
                reached[r, t] = acc
                out.append(acc)
            return tuple(out)

        accs = tuple(jnp.full((8, 128), NEG, jnp.float32) for _ in range(ROWS))
        lax.fori_loop(0, RUN, step, accs, unroll=4)

        for h in (1, 0):
            odd = iota((ROWS * 8, 128), 1)
            tops = []
            group = range(8 * h, 8 * h + 8)
            for d in group:
                tops.append(jnp.concatenate(
                    [reached[r, table_s[r, ENDS + peer_of(d)]] for r in range(ROWS)], axis=0))
            for bit in (4, 2, 1):
                high = (odd // bit) % 2 == 1
                less = []
                for i in range(len(tops) // 2):
                    x, y = tops[i], tops[i + len(tops) // 2]
                    mine = jnp.where(high, y, x)
                    other = jnp.where(high, x, y)
                    other = jnp.where(high, pltpu.roll(other, bit, 1), pltpu.roll(other, 128 - bit, 1))
                    less.append(jnp.maximum(mine, other))
                tops = less
            folded[h] = tops[0].reshape(ROWS, 8, 128)
            ways = [folded[h, :, q, :] for q in range(8)]
            for bit in (4, 2, 1):
                high = (lane // bit) % 2 == 1
                for q in range(8):
                    if q & bit == 0:
                        x, y = ways[q], ways[q + bit]
                        ways[q] = jnp.where(high, pltpu.roll(y, bit, 1), x)
                        ways[q + bit] = jnp.where(high, y, pltpu.roll(x, 128 - bit, 1))
            for p, d in enumerate(group):
                reply[sweep, peer_of(d)] = ways[p]
            for d in ORDER:
                if d in group:
                    rep_copy(sweep, d).start()
        best[sweep, me] = reply[sweep, me]
        for d in FAR:
            root_copy(sweep, d).wait()
        root_sum = jnp.sum(roots[sweep], axis=0)
        price_index = root_sum / (SEC * 2 * ZS)
        price_index = price_index * price_index
        relative = prices / price_index
        wait_all(rep_copy, sweep)
        for s in range(SEC):
            for h in range(2):
                top = best[sweep, 2 * s + h] - 1.41 * capital
                stay = forward[sweep, 2 * s + h] - 0.11 * capital
                gain = jnp.maximum(top, stay)
                rows = slice(h * ROWS, (h + 1) * ROWS)
                live = (survive_ref[s, rows] == 1) & (iota((ROWS, 128), 0) + h * ROWS >= exit_ref[s])
                value_ref[s, rows] = jnp.where(live, relative[s:s + 1] * output[rows] + gain, scrap)
        flat = jnp.where(diagonal, relative, 0.0)
        rel_ref[...] = jnp.sum(flat, axis=0, keepdims=True)[:, :SEC]
        return carry

    lax.fori_loop(0, SWEEPS, sweep_body, 0)


def on_device(start_value, firm_mass, survive, exit_index, demand, transition, install_cost):
    f32 = jnp.float32
    vmem = pl.BlockSpec(memory_space=pltpu.VMEM)
    smem = pl.BlockSpec(memory_space=pltpu.SMEM)
    dma = pltpu.SemaphoreType.DMA
    values, relative = pl.pallas_call(
        kernel,
        out_shape=(jax.ShapeDtypeStruct((SEC, Z, 128), f32), jax.ShapeDtypeStruct((1, SEC), f32)),
        in_specs=[smem, smem] + [pl.BlockSpec(memory_space=pltpu.HBM)] * 5,
        out_specs=(vmem, vmem),
        scratch_shapes=[
            pltpu.VMEM((SWEEPS, CAPS, ROWS, 128), f32),
            pltpu.VMEM((SWEEPS, CAPS, ROWS, 128), f32),
            pltpu.VMEM((GROUPS, ROWS, 128), f32),
            pltpu.VMEM((LINES, 8, 128), f32),
            pltpu.VMEM((ROWS, 128), jnp.int32),
            pltpu.VMEM((ROWS, 128), f32),
            pltpu.SMEM((ROWS, 128), jnp.int32),
            pltpu.SMEM((ROWS, 128), f32),
            pltpu.VMEM((ROWS, RUN, 8, 128), f32),
            pltpu.VMEM((2, ROWS, 8, 128), f32),
            pltpu.VMEM((SWEEPS, CAPS, ROWS, 128), f32),
            pltpu.VMEM((SWEEPS, CAPS, ROWS, 128), f32),
            pltpu.VMEM((SWEEPS, 1, 128), f32),
            pltpu.VMEM((SWEEPS, CAPS, 1, 128), f32),
            pltpu.VMEM((SWEEPS, 1, 128), f32),
            pltpu.VMEM((SWEEPS, 1, 128), f32),
            pltpu.VMEM((SWEEPS, 1, 128), f32),
            pltpu.VMEM((SWEEPS, ZS, 1, 128), f32),
            pltpu.VMEM((SEC, Z, 128), f32),
            pltpu.VMEM((SEC, Z, 128), jnp.int32),
            pltpu.VMEM((Z, Z), f32),
            pltpu.VMEM((1, 128), f32),
            dma((SWEEPS, CAPS)), dma((SWEEPS, CAPS)), dma((SWEEPS, CAPS)), dma((SWEEPS, CAPS)),
            dma((SWEEPS, CAPS)), dma((SWEEPS, CAPS)), dma((SWEEPS,)), dma((SWEEPS,)),
            dma((SWEEPS, ZS)), dma((SWEEPS, ZS)), dma((2,)), dma((5,)),
        ],
        compiler_params=pltpu.CompilerParams(
            collective_id=0, has_side_effects=True, vmem_limit_bytes=(40 << 20)),
    )(exit_index, demand, *(pltpu.with_memory_space_constraint(x, pltpu.HBM) for x in (start_value, firm_mass, survive, transition, install_cost.reshape(1, 128))))
    return values, relative.reshape(SEC)


def solution(mesh):
    placed = (
        P("sector", None, "cap"),
        P("sector", None, "cap"),
        P("sector", None, "cap"),
        P("sector"),
        P("sector"),
        P(),
        P("cap"),
    )
    return jax.shard_map(
        on_device,
        mesh=mesh,
        in_specs=placed,
        out_specs=(P("sector", None, "cap"), P("sector")),
        check_vma=False,
    )
```

```python
import math

import jax
import jax.numpy as jnp
import numpy as np
from jax import lax
from jax.experimental import pallas as pl
from jax.experimental.pallas import tpu as pltpu
from jax.sharding import PartitionSpec as P

K = 2048
Z = 32
SWEEPS = 2
SEC = 8
CAPS = 16
ZS = 16
ROWS = 16
CHUNK = 64
CHUNKS = K // CHUNK
GANG = CHUNK // 8
STEPS = CHUNKS + CAPS - 1
RUN = STEPS + 1
ORDER = sorted(range(1, CAPS), key=lambda d: -sum(min(x, 4 - x) for x in (d // 4, d % 4)))
FAR = sorted(range(1, ZS), key=lambda d: -min(d, ZS - d))
GROUPS = K // 8
LINES = GROUPS + 8 * (CAPS - 1)
SHIFT = 8 * (CAPS - 1)
ENDS = 48
LINE_AT = 64
NEG = -1e30
LOG10 = float(np.log(np.float32(10.0)))


def capital_of(positions):
    return 0.2 * jnp.exp(LOG10 * positions.astype(jnp.float32) / (K - 1))


def iota(shape, axis):
    return lax.broadcasted_iota(jnp.int32, shape, axis)


def kernel(
    exit_ref, demand_ref, start_hbm, mass_hbm, survive_hbm, trans_hbm, install_hbm,
    value_ref, rel_ref,
    forward, heard, heights, lines, table, jumps, table_s, jumps_s,
    reached, folded, reply, best, part, parts, root, pair, both, roots,
    mass_ref, survive_ref, trans_ref, install_ref,
    fwd_send, fwd_recv, rep_send, rep_recv, par_send, par_recv, pair_send, pair_recv,
    root_send, root_recv, table_sem, load_sem,
):
    me = lax.axis_index("cap")
    sec = lax.axis_index("sector")
    core = lax.rem(sec, 2)
    level = sec // 2
    partner = sec + 1 - 2 * core

    row, column = me // 4, lax.rem(me, 4)

    def peer_of(d):
        return 4 * lax.rem(row + d // 4, 4) + lax.rem(column + d % 4, 4)

    def source_of(d):
        return 4 * lax.rem(row + 4 - d // 4, 4) + lax.rem(column + 4 - d % 4, 4)

    def cap_at(d):
        return {"cap": peer_of(d)}

    def level_at(d):
        return {"sector": 2 * lax.rem(level + d, ZS) + core}

    barrier = pltpu.get_barrier_semaphore()

    for d in ORDER:
        pl.semaphore_signal(barrier, inc=1, device_id=cap_at(d))
    for d in FAR:
        pl.semaphore_signal(barrier, inc=1, device_id=level_at(d))
    pl.semaphore_signal(barrier, inc=1, device_id={"sector": partner})

    loads = [
        pltpu.make_async_copy(source, target, load_sem.at[i])
        for i, (source, target) in enumerate((
            (start_hbm, value_ref), (mass_hbm, mass_ref), (survive_hbm, survive_ref),
            (trans_hbm, trans_ref), (install_hbm, install_ref)))
    ]
    for load in loads:
        load.start()

    capital_all = capital_of(iota((CAPS, 128), 0) * 128 + iota((CAPS, 128), 1))
    half = 0.8 * capital_all
    square_all = capital_all * capital_all
    low = iota((8, 128), 1) % 8
    own_place = 2 * low - 8 * (iota((8, 128), 1) // 8) - iota((8, 128), 0)

    def fill(i, c):
        lines[i] = capital_of(16 * (i - SHIFT) + own_place)
        return c

    lax.fori_loop(0, LINES, fill, 0, unroll=8)
    place = me * 128 + iota((1, 128), 1)
    capital = capital_of(place)
    scrap = 0.3 * capital
    log_cap = math.log(0.2) + LOG10 * place.astype(jnp.float32) / (K - 1)
    log_prod = -0.5 + iota((Z, 128), 0).astype(jnp.float32) / (Z - 1)
    output = jnp.exp(log_prod + 0.6 * log_cap)
    lane = iota((ROWS, 128), 1)
    lane_f = lane.astype(jnp.float32)

    def fwd_copy(sweep, d):
        peer = peer_of(d)
        return pltpu.make_async_remote_copy(
            forward.at[sweep, peer], heard.at[sweep, me], fwd_send.at[sweep, d], fwd_recv.at[sweep, d],
            device_id=cap_at(d))

    def rep_copy(sweep, d):
        peer = peer_of(d)
        return pltpu.make_async_remote_copy(
            reply.at[sweep, peer], best.at[sweep, me], rep_send.at[sweep, d], rep_recv.at[sweep, d],
            device_id=cap_at(d))

    def par_copy(sweep, d):
        return pltpu.make_async_remote_copy(
            part.at[sweep], parts.at[sweep, me], par_send.at[sweep, d], par_recv.at[sweep, d],
            device_id=cap_at(d))

    def root_copy(sweep, d):
        return pltpu.make_async_remote_copy(
            both.at[sweep], roots.at[sweep, level], root_send.at[sweep, d], root_recv.at[sweep, d],
            device_id=level_at(d))

    def start_all(copy, sweep):
        for d in ORDER:
            copy(sweep, d).start()

    def wait_all(copy, sweep):
        for d in ORDER:
            copy(sweep, d).wait()

    for load in loads:
        load.wait()
    install = install_ref[...]

    def sweep_body(sweep, carry):
        sums = []
        for s in range(SEC):
            live = (survive_ref[s] == 1) & (iota((Z, 128), 0) >= exit_ref[s])
            values = value_ref[s]
            staying = jnp.where(live, jax.nn.sigmoid((values - scrap) * 2.0), 0.0)
            sums.append(jnp.sum(mass_ref[s] * staying * output, axis=0, keepdims=True))
            continuation = jnp.where(live, jnp.maximum(values, scrap), scrap)
            expect = lax.dot_general(
                trans_ref[...], continuation, (((1,), (0,)), ((), ())),
                precision=lax.Precision.HIGHEST, preferred_element_type=jnp.float32)
            ahead = 0.9 * expect - install
            forward[sweep, 2 * s] = ahead[:ROWS]
            forward[sweep, 2 * s + 1] = ahead[ROWS:]
        sums = jnp.sum(jnp.concatenate(sums, axis=0), axis=1, keepdims=True)
        diagonal = iota((SEC, 128), 0) == iota((SEC, 128), 1)
        part[sweep] = jnp.sum(jnp.where(diagonal, sums, 0.0), axis=0, keepdims=True)

        @pl.when(sweep == 0)
        def _():
            pl.semaphore_wait(barrier, CAPS - 1 + ZS - 1 + 1)

        start_all(par_copy, sweep)
        start_all(fwd_copy, sweep)
        heard[sweep, me] = forward[sweep, me]
        parts[sweep, me] = part[sweep]
        def spread(i):
            rows = [heard[sweep, i] + 0.8 * capital_of(i * 128 + iota((1, 128), 1))]
            for bit in (64, 32, 16, 8):
                high = (lane // bit) % 2 == 1
                wide = []
                for x in rows:
                    turned = pltpu.roll(x, bit, 1)
                    wide += [jnp.where(high, turned, x), jnp.where(high, x, turned)]
                rows = wide
            for g in range(16):
                heights[16 * i + g] = rows[g]

        wait_all(fwd_copy, sweep)

        tall = heard[sweep] + half[:, None, :]
        source = lax.broadcasted_iota(jnp.int32, (CAPS, ROWS, 128), 0).astype(jnp.float32)
        chunks = []
        for b in range(1, CAPS):
            rate = 1.0 / (0.2 * math.exp(LOG10 * 128 * b / (K - 1)))
            here = tall - (square_all * rate)[:, None, :]
            top = jnp.max(here, axis=0)
            where = jnp.min(jnp.where(here == top[None], source, 1e9), axis=0)
            peak = jnp.max(top, axis=1, keepdims=True)
            spot = where * (128 // CHUNK) + (lane // CHUNK).astype(jnp.float32)
            chunk = jnp.min(jnp.where(top == peak, spot, 1e9), axis=1, keepdims=True)
            chunk = jnp.broadcast_to(chunk, (ROWS, 128))
            chunks.append(jnp.maximum(chunk, chunks[-1]) if chunks else chunk)
        chunks.append(jnp.full((ROWS, 128), float(CHUNKS - 1), jnp.float32))
        block = jnp.zeros((ROWS, 128), jnp.float32)
        jump = jnp.zeros((ROWS, 128), jnp.float32)
        time = lane_f - jnp.where(lane < LINE_AT, 0.0, float(LINE_AT))
        for b in range(1, CAPS):
            first = chunks[b - 1] + float(b)
            block = block + jnp.where(first <= time, 1.0, 0.0)
            jump = jnp.where(first == time, NEG, jump)
        entry = float(GANG) * (time - block)
        entry = entry + jnp.where(lane < LINE_AT, 0.0, float(SHIFT) - 8.0 * block)
        for b in range(CAPS):
            entry = jnp.where(lane == ENDS + b, chunks[b] + float(b), entry)
        limit = jnp.where(lane < ENDS, GROUPS - GANG, jnp.where(lane < LINE_AT, STEPS - 1, LINES - GANG))
        table[...] = jnp.clip(entry.astype(jnp.int32), 0, limit)
        jumps[...] = jump
        to_table = pltpu.make_async_copy(table, table_s, table_sem.at[0])
        to_jumps = pltpu.make_async_copy(jumps, jumps_s, table_sem.at[1])
        to_table.start()
        to_jumps.start()
        wait_all(par_copy, sweep)
        whole = jnp.sum(jnp.where(diagonal, jnp.sum(parts[sweep], axis=0), 0.0), axis=1, keepdims=True)
        supply = 1.0 + jnp.broadcast_to(whole, (SEC, 128)) / (Z * K)
        demand = jnp.zeros((SEC, 128), jnp.float32)
        for s in range(SEC):
            demand = jnp.where(iota((SEC, 128), 0) == s, demand_ref[s], demand)
        prices = jnp.sqrt(demand / supply)
        root[sweep] = jnp.sum(jnp.sqrt(prices), axis=0, keepdims=True)
        to_pair = pltpu.make_async_remote_copy(
            root.at[sweep], pair.at[sweep], pair_send.at[sweep], pair_recv.at[sweep],
            device_id={"sector": partner})
        to_pair.start()
        spread(me)
        for d in ORDER:
            spread(source_of(d))
        to_pair.wait()
        both[sweep] = root[sweep] + pair[sweep]
        for d in FAR:
            root_copy(sweep, d).start()
        roots[sweep, level] = both[sweep]
        to_table.wait()
        to_jumps.wait()

        def step(t, accs):
            out = []
            for r in range(ROWS):
                value = heights[pl.ds(table_s[r, t], GANG), r:r + 1, :] - lines[pl.ds(table_s[r, LINE_AT + t], GANG)]
                acc = jnp.maximum(jnp.max(value, axis=0), accs[r] + jumps_s[r, t])
                reached[r, t] = acc
                out.append(acc)
            return tuple(out)

        accs = tuple(jnp.full((8, 128), NEG, jnp.float32) for _ in range(ROWS))
        lax.fori_loop(0, RUN, step, accs, unroll=4)

        for h in (1, 0):
            odd = iota((ROWS * 8, 128), 1)
            tops = []
            group = range(8 * h, 8 * h + 8)
            for d in group:
                tops.append(jnp.concatenate(
                    [reached[r, table_s[r, ENDS + peer_of(d)]] for r in range(ROWS)], axis=0))
            for bit in (4, 2, 1):
                high = (odd // bit) % 2 == 1
                less = []
                for i in range(len(tops) // 2):
                    x, y = tops[i], tops[i + len(tops) // 2]
                    mine = jnp.where(high, y, x)
                    other = jnp.where(high, x, y)
                    other = jnp.where(high, pltpu.roll(other, bit, 1), pltpu.roll(other, 128 - bit, 1))
                    less.append(jnp.maximum(mine, other))
                tops = less
            folded[h] = tops[0].reshape(ROWS, 8, 128)
            ways = [folded[h, :, q, :] for q in range(8)]
            for bit in (4, 2, 1):
                high = (lane // bit) % 2 == 1
                for q in range(8):
                    if q & bit == 0:
                        x, y = ways[q], ways[q + bit]
                        ways[q] = jnp.where(high, pltpu.roll(y, bit, 1), x)
                        ways[q + bit] = jnp.where(high, y, pltpu.roll(x, 128 - bit, 1))
            for p, d in enumerate(group):
                reply[sweep, peer_of(d)] = ways[p]
            for d in ORDER:
                if d in group:
                    rep_copy(sweep, d).start()
        best[sweep, me] = reply[sweep, me]
        for d in FAR:
            root_copy(sweep, d).wait()
        root_sum = jnp.sum(roots[sweep], axis=0)
        price_index = root_sum / (SEC * 2 * ZS)
        price_index = price_index * price_index
        relative = prices / price_index
        wait_all(rep_copy, sweep)
        for s in range(SEC):
            for h in range(2):
                top = best[sweep, 2 * s + h] - 1.41 * capital
                stay = forward[sweep, 2 * s + h] - 0.11 * capital
                gain = jnp.maximum(top, stay)
                rows = slice(h * ROWS, (h + 1) * ROWS)
                live = (survive_ref[s, rows] == 1) & (iota((ROWS, 128), 0) + h * ROWS >= exit_ref[s])
                value_ref[s, rows] = jnp.where(live, relative[s:s + 1] * output[rows] + gain, scrap)
        flat = jnp.where(diagonal, relative, 0.0)
        rel_ref[...] = jnp.sum(flat, axis=0, keepdims=True)[:, :SEC]
        return carry

    lax.fori_loop(0, SWEEPS, sweep_body, 0)


def on_device(start_value, firm_mass, survive, exit_index, demand, transition, install_cost):
    f32 = jnp.float32
    vmem = pl.BlockSpec(memory_space=pltpu.VMEM)
    smem = pl.BlockSpec(memory_space=pltpu.SMEM)
    dma = pltpu.SemaphoreType.DMA
    values, relative = pl.pallas_call(
        kernel,
        out_shape=(jax.ShapeDtypeStruct((SEC, Z, 128), f32), jax.ShapeDtypeStruct((1, SEC), f32)),
        in_specs=[smem, smem] + [pl.BlockSpec(memory_space=pltpu.HBM)] * 5,
        out_specs=(vmem, vmem),
        scratch_shapes=[
            pltpu.VMEM((SWEEPS, CAPS, ROWS, 128), f32),
            pltpu.VMEM((SWEEPS, CAPS, ROWS, 128), f32),
            pltpu.VMEM((GROUPS, ROWS, 128), f32),
            pltpu.VMEM((LINES, 8, 128), f32),
            pltpu.VMEM((ROWS, 128), jnp.int32),
            pltpu.VMEM((ROWS, 128), f32),
            pltpu.SMEM((ROWS, 128), jnp.int32),
            pltpu.SMEM((ROWS, 128), f32),
            pltpu.VMEM((ROWS, RUN, 8, 128), f32),
            pltpu.VMEM((2, ROWS, 8, 128), f32),
            pltpu.VMEM((SWEEPS, CAPS, ROWS, 128), f32),
            pltpu.VMEM((SWEEPS, CAPS, ROWS, 128), f32),
            pltpu.VMEM((SWEEPS, 1, 128), f32),
            pltpu.VMEM((SWEEPS, CAPS, 1, 128), f32),
            pltpu.VMEM((SWEEPS, 1, 128), f32),
            pltpu.VMEM((SWEEPS, 1, 128), f32),
            pltpu.VMEM((SWEEPS, 1, 128), f32),
            pltpu.VMEM((SWEEPS, ZS, 1, 128), f32),
            pltpu.VMEM((SEC, Z, 128), f32),
            pltpu.VMEM((SEC, Z, 128), jnp.int32),
            pltpu.VMEM((Z, Z), f32),
            pltpu.VMEM((1, 128), f32),
            dma((SWEEPS, CAPS)), dma((SWEEPS, CAPS)), dma((SWEEPS, CAPS)), dma((SWEEPS, CAPS)),
            dma((SWEEPS, CAPS)), dma((SWEEPS, CAPS)), dma((SWEEPS,)), dma((SWEEPS,)),
            dma((SWEEPS, ZS)), dma((SWEEPS, ZS)), dma((2,)), dma((5,)),
        ],
        compiler_params=pltpu.CompilerParams(
            collective_id=0, has_side_effects=True, vmem_limit_bytes=(40 << 20)),
    )(exit_index, demand, *(pltpu.with_memory_space_constraint(x, pltpu.HBM) for x in (start_value, firm_mass, survive, transition, install_cost.reshape(1, 128))))
    return values, relative.reshape(SEC)


def solution(mesh):
    placed = (
        P("sector", None, "cap"),
        P("sector", None, "cap"),
        P("sector", None, "cap"),
        P("sector"),
        P("sector"),
        P(),
        P("cap"),
    )
    return jax.shard_map(
        on_device,
        mesh=mesh,
        in_specs=placed,
        out_specs=(P("sector", None, "cap"), P("sector")),
        check_vma=False,
    )
```
